256 devices in a mesh: dp: 16 (over z, core), expert: 16 (over y, x).
Axes of the slice: x: 4, y: 4, z: 8, core: 2. Of those that a mesh axis runs over, the one named last changes fastest.
Arguments:
- tokens: bfloat16 [131072, 2048], P(('dp', 'expert')), parts along dimension 0, may hold values from -6 to 6
- modality: int32 [131072], P(('dp', 'expert')), parts along dimension 0, may hold values 0 or 1
- expert_ids: int32 [131072, 2], P(('dp', 'expert')), parts along dimension 0, may hold values from 0 to 15, all different within a row; in each aligned block of 512 rows (0 to 511, 512 to 1023, ...) at most 80 rows name the same one
- route_weights: float32 [131072, 2], P(('dp', 'expert')), parts along dimension 0, may hold values from 0.25 to 1
- norm_gain: float32 [2, 2048], replicated, may hold values from 0.25 to 1.75
- gate_weight: bfloat16 [2048, 14336], P(None, 'expert'), may hold values from -0.125 to 0.125
- up_weight: bfloat16 [2048, 14336], P(None, 'expert'), may hold values from -0.125 to 0.125
- down_weight: bfloat16 [14336, 2048], P('expert'), may hold values from -0.1875 to 0.1875
Outputs:
- mixed: bfloat16 [131072, 2048], P(('dp', 'expert')), parts along dimension 0
The draws below stay inside these ranges and needn't reach their ends.
There are 16 independent parts, one for each index of `dp`. The reference program is written for one: setup_inputs(seed, part) draws one part's arguments, and reference() takes and returns one part's arrays. A program takes and returns all parts, laid end to end along the dimension named above; an argument that names none is the same for every part. Nothing has to cross between parts.
Inputs may be any that keep to these rules, and one draw needn't show every extreme that they name: `expert_ids`: each row names 2 different experts. Among the rows of one device no expert is named by more than 80 rows, a bound that some blocks reach.
All inputs are finite; a program needn't handle non-finite values. No bound on the sum of `modality` on one device may be relied on, other than what follows from the above.
Results may differ from the reference program's by a relative error of at most 0.0054.
Values may be sent and summed in bfloat16 or wider, within the bound.
A program may use at most 128 MiB of HBM per device.

```python
import math
import jax
import jax.numpy as jnp
import numpy as np
from jax import lax

D = 2048
HIDDEN_SIZE = 896
TOP = 2
TOK_DEV = 512
EXPERTS = 16
CAP = 80
TOKENS = 8192
N_EXPERT = 16


def set_ends(result, stream_key, low, largest):
    dims = result.shape
    index_at = [jax.random.randint(jax.random.fold_in(stream_key, axis), (), 0, dims[axis]) for axis in range(len(dims))]
    result = result.at[tuple(index_at)].set(low)
    longest = dims.index(max(dims))
    index_at[longest] = (index_at[longest] + 1) % dims[longest]
    return result.at[tuple(index_at)].set(largest)


def block_scale(own_key, shape, shards, least, high):
    def one(dim, shards_of):
        steps = jax.random.uniform(jax.random.fold_in(jax.random.fold_in(own_key, 6), dim), (shards_of,), jnp.float32, least / len(shards), high / len(shards))
        return jnp.repeat(jnp.exp(steps), shape[dim] // shards_of).reshape((-1,) + (1,) * (len(shape) - dim - 1))

    gain = one(*shards[0])
    for cut in shards[1:]:
        gain = gain * one(*cut)
    return gain


def deal_out(key, own, number, rows, count, top, limit, lean):
    order = jax.random.permutation(key, count)
    heavy_load, ordinary = shares(count, rows * top, limit, lean, True), shares(count, rows * top, limit, lean, False)
    places = jnp.arange(count)

    def named(sizes, offset_by):
        used = int((sizes > 0).sum())
        fixed = max(1, used // 4)
        moved = fixed + (places - fixed + offset_by * (used - fixed)) % max(1, count - fixed)
        return jnp.zeros((count,), jnp.int32).at[order[jnp.where(places < fixed, places, moved)]].set(jnp.asarray(sizes, jnp.int32))

    sizes = jnp.where(number % 4 == 0, named(heavy_load, number // 4), named(ordinary, number - number // 4 - 1))
    mixed = jax.random.permutation(jax.random.fold_in(own, 3), count)
    source_of, taker = mixed[0:count // 2 * 2:2], mixed[1:count // 2 * 2:2]
    room = jnp.minimum(sizes[source_of] - 1, limit - sizes[taker]) // 2
    room = jnp.where((source_of == order[0]) | (taker == order[0]) | (sizes[taker] == 0), 0, jnp.maximum(room, 0))
    moved = jax.random.randint(jax.random.fold_in(own, 4), (count // 2,), 0, 1 << 20) % (room + 1)
    sizes = sizes.at[source_of].add(-moved).at[taker].add(moved)
    labels = jnp.searchsorted(jnp.cumsum(sizes), jnp.arange(rows * top), side="right").astype(jnp.int32)
    table = labels.reshape(top, rows).T
    table = table[jax.random.permutation(jax.random.fold_in(own, 1), rows)]
    offset_by = jax.random.randint(jax.random.fold_in(own, 2), (rows, 1), 0, top)
    return jnp.take_along_axis(table, (jnp.arange(top)[None, :] + offset_by) % top, axis=1)


def shares(number_of, total, bound, slope, full):
    loads = [(1 << 20) // math.isqrt(rank ** slope) + 1 for rank in range(1, number_of + 1)]
    largest = bound if full else min(bound, max(-(-total // number_of), total * loads[0] // sum(loads)))
    least = 1 if total - largest >= number_of - 1 else 0
    counts, rest = [largest] + [least] * (number_of - 1), total - largest - least * (number_of - 1)
    while rest > 0:
        free = [i for i in range(1, number_of) if counts[i] < largest] or [i for i in range(1, number_of) if counts[i] < bound]
        pool, budget = sum([loads[i] for i in free]), rest
        for i in free:
            extra = min(bound - counts[i], max(1, budget * loads[i] // pool), rest)
            counts[i] = counts[i] + extra
            rest = rest - extra
    return np.array(counts)


def bell_draw(stream_key, shape, spread, most, split=(), held_as=jnp.bfloat16):
    factor_of = block_scale(stream_key, shape, split, -0.22, 0.18) if split else 1.0
    result = jax.random.normal(stream_key, shape, jnp.float32) * spread * factor_of
    return jnp.minimum(jnp.maximum(result, -most), most).astype(held_as)


def setup_inputs(seed: int = 0, part: int = 0) -> dict:
    key_list = jax.random.split(jax.random.key(seed), 9)
    part_splits = jax.random.split(jax.random.fold_in(key_list[8], part), 9)
    tokens = bell_draw(part_splits[0], (TOKENS, D), 1.0, 6.0, ((0, 16),))
    modality = set_ends((jax.random.randint(part_splits[1], (TOKENS,), 0, 2) < 1).astype(jnp.int32), jax.random.fold_in(part_splits[1], 1), 0, 1)
    expert_ids_keys = jax.random.split(jax.random.fold_in(part_splits[2], 1), TOKENS // TOK_DEV)
    expert_ids_turns = jax.random.permutation(jax.random.fold_in(part_splits[2], 3), TOKENS // TOK_DEV)
    expert_ids = jax.vmap(lambda own, number: deal_out(jax.random.fold_in(part_splits[2], 2), own, number, TOK_DEV, EXPERTS, TOP, CAP, 1))(expert_ids_keys, expert_ids_turns).reshape((TOKENS, TOP))
    route_weights = jnp.clip(0.25 + 0.75 * jax.random.uniform(part_splits[3], (TOKENS, TOP), jnp.float32) ** block_scale(part_splits[3], (TOKENS, TOP), ((0, 16),), -0.2, 0.2), 0.25, 1.0)
    norm_gain = jnp.clip(1.0 + 0.15 * jax.random.normal(key_list[4], (2, D), jnp.float32), 0.25, 1.75)
    gate_weight = bell_draw(key_list[5], (D, EXPERTS * HIDDEN_SIZE), D ** -0.5, 0.125, ((1, 16),))
    up_weight = bell_draw(key_list[6], (D, EXPERTS * HIDDEN_SIZE), D ** -0.5, 0.125, ((1, 16),))
    down_weight = bell_draw(key_list[7], (EXPERTS * HIDDEN_SIZE, D), HIDDEN_SIZE ** -0.5, 0.1875, ((0, 16),))
    return dict(tokens=tokens, modality=modality, expert_ids=expert_ids, route_weights=route_weights, norm_gain=norm_gain, gate_weight=gate_weight, up_weight=up_weight, down_weight=down_weight)


epsilon = 1e-05

def normalize(tokens, modality, norm_gain):
    values = tokens.astype(jnp.float32)
    square = lax.optimization_barrier(jnp.mean(values * values, axis=1, keepdims=True))
    gains = jnp.where(modality[:, None] == 1, norm_gain[1][None, :], norm_gain[0][None, :])
    return (values * lax.rsqrt(square + epsilon) * gains).astype(jnp.bfloat16)

def slot_table(expert_ids, experts, capacity):
    fanout = expert_ids.shape[1]
    flat_ids = expert_ids.reshape(-1).astype(jnp.int32)
    columns = jnp.arange(experts, dtype=jnp.int32)
    onehot = (flat_ids[:, None] == columns[None, :]).astype(jnp.int32)
    earlier = jnp.cumsum(onehot, axis=0).astype(jnp.int32) - onehot
    position = lax.optimization_barrier(jnp.sum(earlier * onehot, axis=1)).astype(jnp.int32)
    slots = (flat_ids * capacity + position).astype(jnp.int32)
    sources = (jnp.arange(flat_ids.shape[0], dtype=jnp.int32) // fanout).astype(jnp.int32)
    owners = jnp.full((experts * capacity,), -1, jnp.int32).at[slots].set(sources)
    return (slots, owners)

def pack_rows(normed, owners):
    chosen = jnp.take(normed, jnp.maximum(owners, 0), axis=0)
    return jnp.where(owners[:, None] >= 0, chosen, jnp.zeros_like(chosen))

def expert_rows(rows, gate_cols, up_cols, down_rows):
    gate = jnp.dot(rows, gate_cols, preferred_element_type=jnp.float32)
    upper = jnp.dot(rows, up_cols, preferred_element_type=jnp.float32)
    active = (jax.nn.silu(gate) * upper).astype(jnp.bfloat16)
    return jnp.dot(active, down_rows, preferred_element_type=jnp.float32)

def reference(tokens, modality, expert_ids, route_weights, norm_gain, gate_weight, up_weight, down_weight):
    normed = normalize(tokens, modality, norm_gain)
    block_normed = normed.reshape(N_EXPERT, TOK_DEV, D)
    block_ids = expert_ids.reshape(N_EXPERT, TOK_DEV, TOP)
    slots, owners = jax.vmap(lambda ids: slot_table(ids, EXPERTS, CAP))(block_ids)
    packed = jax.vmap(pack_rows)(block_normed, owners)
    per_expert = packed.reshape(N_EXPERT, EXPERTS, CAP, D).transpose(1, 0, 2, 3).reshape(EXPERTS, N_EXPERT * CAP, D)

    def run_one(index):
        start = (index * HIDDEN_SIZE).astype(jnp.int32)
        gate_cols = lax.dynamic_slice_in_dim(gate_weight, start, HIDDEN_SIZE, 1)
        up_cols = lax.dynamic_slice_in_dim(up_weight, start, HIDDEN_SIZE, 1)
        down_rows = lax.dynamic_slice_in_dim(down_weight, start, HIDDEN_SIZE, 0)
        rows = lax.dynamic_index_in_dim(per_expert, index, 0, keepdims=False)
        return expert_rows(rows, gate_cols, up_cols, down_rows).astype(jnp.bfloat16)
    outputs = lax.map(run_one, jnp.arange(EXPERTS, dtype=jnp.int32))
    by_block = outputs.reshape(EXPERTS, N_EXPERT, CAP, D).transpose(1, 0, 2, 3).reshape(N_EXPERT, EXPERTS * CAP, D)
    picked = jax.vmap(lambda table, where_to: jnp.take(table, where_to, axis=0))(by_block, slots)
    picked = picked.reshape(TOKENS, TOP, D).astype(jnp.float32)
    mixed = tokens.astype(jnp.float32) + lax.optimization_barrier(jnp.sum(route_weights[:, :, None] * picked, axis=1))
    return mixed.astype(jnp.bfloat16)
```

```python
import functools

import jax
import jax.numpy as jnp
from jax import lax
from jax.experimental import pallas as pl
from jax.experimental.pallas import tpu as pltpu
from jax.sharding import PartitionSpec as P

MESH = pl.DeviceIdType.MESH
epsilon = 1e-05
SIDE = 4
BLOCKS = 16
GROUP = 4
CHUNK = 16
OFFSETS = (
    (0, 0), (2, 2), (1, 2), (3, 2),
    (2, 1), (2, 3), (1, 1), (3, 3),
    (1, 3), (3, 1), (2, 0), (0, 2),
    (1, 0), (3, 0), (0, 1), (0, 3),
)


def kernel(
    cap, tokens_hbm, meta_ref, gain_ref, gate_hbm, up_hbm, down_hbm, out_ref,
    tokens, normed, cols, slots, send, recv, res, ret, wgu, wd, act, acc,
    load_sem, gu_sem, send_sem, recv_sem, back_sem, ret_sem,
):
    rows, width = tokens.shape
    hidden = wd.shape[0]
    tiles = hidden // 128
    groups = BLOCKS // GROUP
    span = GROUP * cap
    me = lax.axis_index("expert")
    ex, ey = me % SIDE, me // SIDE

    def peer(i, sign):
        dx, dy = OFFSETS[i]
        return ((ey + sign * dy + SIDE) % SIDE) * SIDE + (ex + sign * dx + SIDE) % SIDE

    barrier = pltpu.get_barrier_semaphore()
    for i in range(1, BLOCKS):
        pl.semaphore_signal(barrier, inc=1, device_id={"expert": peer(i, 1)}, device_id_type=MESH)

    load = pltpu.make_async_copy(tokens_hbm, tokens, load_sem.at[0])
    load.start()
    loads = []
    for t in range(tiles):
        for half, source in enumerate((gate_hbm, up_hbm)):
            loads.append(
                pltpu.make_async_copy(
                    source.at[:, pl.ds(t * 128, 128)],
                    wgu.at[:, pl.ds(t * 256 + half * 128, 128)],
                    gu_sem.at[2 * t + half],
                )
            )
    loads.append(pltpu.make_async_copy(down_hbm, wd, load_sem.at[1]))
    for copy in loads:
        copy.start()

    id0, id1 = meta_ref[0:1, :], meta_ref[1:2, :]
    w0, w1 = meta_ref[2:3, :], meta_ref[3:4, :]
    experts = lax.broadcasted_iota(jnp.int32, (BLOCKS, rows), 0).astype(jnp.float32)
    is0, is1 = experts == id0, experts == id1
    names = jnp.where(is0 | is1, 1.0, 0.0).astype(jnp.bfloat16)
    before = lax.broadcasted_iota(jnp.int32, (rows, rows), 0) < lax.broadcasted_iota(jnp.int32, (rows, rows), 1)
    earlier = jnp.dot(names, jnp.where(before, 1.0, 0.0).astype(jnp.bfloat16), preferred_element_type=jnp.float32)
    pos0 = jnp.sum(jnp.where(is0, earlier, 0.0), axis=0, keepdims=True)
    pos1 = jnp.sum(jnp.where(is1, earlier, 0.0), axis=0, keepdims=True)
    base0, base1 = jnp.zeros_like(id0), jnp.zeros_like(id1)
    for i in range(1, BLOCKS):
        name = peer(i, 1).astype(jnp.float32)
        base0 = jnp.where(id0 == name, float(i * cap), base0)
        base1 = jnp.where(id1 == name, float(i * cap), base1)
    slot0, slot1 = base0 + pos0, base1 + pos1
    hi0, hi1 = w0.astype(jnp.bfloat16).astype(jnp.float32), w1.astype(jnp.bfloat16).astype(jnp.float32)
    slots[0:1, :] = slot0.astype(jnp.int32)
    slots[1:2, :] = slot1.astype(jnp.int32)
    table = jnp.concatenate([slot0, slot1, hi0, hi1, w0 - hi0, w1 - hi1, meta_ref[4:5, :], jnp.zeros_like(id0)], axis=0)
    cols[...] = jnp.concatenate([table, jnp.zeros((120, rows), jnp.float32)], axis=0).T

    load.wait()
    step = 64

    def norm_step(r, carry):
        at = pl.ds(pl.multiple_of(r * step, step), step)
        values = tokens[at, :].astype(jnp.float32)
        square = jnp.mean(values * values, axis=1, keepdims=True)
        gains = jnp.where(cols[at, 6:7] == 1.0, gain_ref[1:2, :], gain_ref[0:1, :])
        normed[at, :] = (values * lax.rsqrt(square + epsilon) * gains).astype(jnp.bfloat16)
        return carry

    lax.fori_loop(0, rows // step, norm_step, 0)

    def parts(source, target, sems, rsems, i, device):
        return [
            pltpu.make_async_remote_copy(
                src_ref=source.at[i, pl.ds(c * CHUNK, CHUNK), :],
                dst_ref=target.at[i, pl.ds(c * CHUNK, CHUNK), :],
                send_sem=sems.at[i],
                recv_sem=rsems.at[i],
                device_id={"expert": device},
                device_id_type=MESH,
            )
            for c in range(cap // CHUNK)
        ]

    def whole(source, target, sems, rsems, i, device):
        return pltpu.make_async_remote_copy(
            src_ref=source.at[i],
            dst_ref=target.at[i],
            send_sem=sems.at[i],
            recv_sem=rsems.at[i],
            device_id={"expert": device},
            device_id_type=MESH,
        )

    def start_all(source, target, sems, rsems, blocks, sign):
        lists = [parts(source, target, sems, rsems, i, peer(i, sign)) for i in blocks]
        for c in range(cap // CHUNK):
            for copies in lists:
                copies[c].start()

    for g in range(groups):
        place = lax.broadcasted_iota(jnp.int32, (span, rows), 0) + g * span
        pick = jnp.where((place == slots[0:1, :]) | (place == slots[1:2, :]), 1.0, 0.0).astype(jnp.bfloat16)
        half = width // 4

        def pack_step(n, carry):
            at = pl.ds(pl.multiple_of(n * half, half), half)
            packed = jnp.dot(pick, normed[:, at], preferred_element_type=jnp.float32).astype(jnp.bfloat16)
            packed = packed.reshape(GROUP, cap, half)
            if g == 0:
                recv[0:1, :, at] = packed[0:1]
                send[1:GROUP, :, at] = packed[1:]
            else:
                send[g * GROUP : (g + 1) * GROUP, :, at] = packed
            return carry

        lax.fori_loop(0, 4, pack_step, 0)
        if g == 0:
            pl.semaphore_wait(barrier, BLOCKS - 1)
        start_all(send, recv, send_sem, recv_sem, [i for i in range(g * GROUP, (g + 1) * GROUP) if i], 1)

    for copy in loads:
        copy.wait()

    for g in range(groups):
        blocks = [i for i in range(g * GROUP, (g + 1) * GROUP) if i]
        for i in blocks:
            whole(send, recv, send_sem, recv_sem, i, peer(i, 1)).wait_recv()

        def hidden_step(t, carry):
            at = pl.ds(pl.multiple_of(t * 256, 256), 256)
            flat = recv[g * GROUP : (g + 1) * GROUP].reshape(span, width)
            both = jnp.dot(flat, wgu[:, at], preferred_element_type=jnp.float32)
            gate, upper = both[:, :128], both[:, 128:]
            act[:, pl.ds(pl.multiple_of(t * 128, 128), 128)] = (jax.nn.silu(gate) * upper).astype(jnp.bfloat16)
            return carry

        lax.fori_loop(0, tiles, hidden_step, 0)

        def down_step(n, carry):
            at = pl.ds(pl.multiple_of(n * 256, 256), 256)
            done = jnp.dot(act[...], wd[:, at], preferred_element_type=jnp.float32).astype(jnp.bfloat16)
            done = done.reshape(GROUP, cap, 256)
            if g == 0:
                ret[0:1, :, at] = done[0:1]
                res[1:GROUP, :, at] = done[1:]
            else:
                res[g * GROUP : (g + 1) * GROUP, :, at] = done
            return carry

        lax.fori_loop(0, width // 256, down_step, 0)
        start_all(res, ret, back_sem, ret_sem, blocks, -1)

    for g in range(groups):
        blocks = [i for i in range(g * GROUP, (g + 1) * GROUP) if i]
        for i in blocks:
            whole(res, ret, back_sem, ret_sem, i, peer(i, -1)).wait_recv()
        place = (lax.broadcasted_iota(jnp.int32, (rows, span), 1) + g * span).astype(jnp.float32)
        at0, at1 = place == cols[:, 0:1], place == cols[:, 1:2]
        high = (jnp.where(at0, cols[:, 2:3], 0.0) + jnp.where(at1, cols[:, 3:4], 0.0)).astype(jnp.bfloat16)
        low = (jnp.where(at0, cols[:, 4:5], 0.0) + jnp.where(at1, cols[:, 5:6], 0.0)).astype(jnp.bfloat16)

        def mix_step(n, carry):
            at = pl.ds(pl.multiple_of(n * 256, 256), 256)
            block = ret[g * GROUP : (g + 1) * GROUP, :, at].reshape(span, 256)
            total = jnp.dot(high, block, preferred_element_type=jnp.float32)
            total = total + jnp.dot(low, block, preferred_element_type=jnp.float32)
            if g > 0:
                total = total + acc[:, at]
            if g < groups - 1:
                acc[:, at] = total
            else:
                out_ref[:, at] = (tokens[:, at].astype(jnp.float32) + total).astype(jnp.bfloat16)
            return carry

        lax.fori_loop(0, width // 256, mix_step, 0)

    for i in range(1, BLOCKS):
        whole(send, recv, send_sem, recv_sem, i, peer(i, 1)).wait_send()
        whole(res, ret, back_sem, ret_sem, i, peer(i, -1)).wait_send()


def shards(tokens, modality, expert_ids, route_weights, norm_gain, gate_weight, up_weight, down_weight):
    rows, width = tokens.shape
    fanout = expert_ids.shape[1]
    hidden = down_weight.shape[0]
    cap = min(rows, rows * fanout * 5 // (4 * BLOCKS))
    meta = jnp.concatenate(
        [
            expert_ids.T.astype(jnp.float32),
            route_weights.T,
            modality[None, :].astype(jnp.float32),
            jnp.zeros((3, rows), jnp.float32),
        ],
        axis=0,
    )
    anywhere = pl.BlockSpec(memory_space=pl.ANY)
    vmem = pl.BlockSpec(memory_space=pltpu.VMEM)
    block = pltpu.VMEM((BLOCKS, cap, width), jnp.bfloat16)
    sems = pltpu.SemaphoreType.DMA((BLOCKS,))
    return pl.pallas_call(
        functools.partial(kernel, cap),
        out_shape=jax.ShapeDtypeStruct((rows, width), jnp.bfloat16),
        in_specs=[anywhere, vmem, vmem, anywhere, anywhere, anywhere],
        out_specs=vmem,
        scratch_shapes=[
            pltpu.VMEM((rows, width), jnp.bfloat16),
            pltpu.VMEM((rows, width), jnp.bfloat16),
            pltpu.VMEM((rows, 128), jnp.float32),
            pltpu.VMEM((8, rows), jnp.int32),
            block, block, block, block,
            pltpu.VMEM((width, 2 * hidden), jnp.bfloat16),
            pltpu.VMEM((hidden, width), jnp.bfloat16),
            pltpu.VMEM((GROUP * cap, hidden), jnp.bfloat16),
            pltpu.VMEM((rows, width), jnp.float32),
            pltpu.SemaphoreType.DMA((2,)),
            pltpu.SemaphoreType.DMA((2 * (hidden // 128),)),
            sems, sems, sems, sems,
        ],
        compiler_params=pltpu.CompilerParams(
            collective_id=0, has_side_effects=True, vmem_limit_bytes=62 * 1024 * 1024
        ),
    )(tokens, meta, norm_gain, gate_weight, up_weight, down_weight)


def solution(mesh):
    placed = (
        P(("dp", "expert"), None),
        P(("dp", "expert")),
        P(("dp", "expert"), None),
        P(("dp", "expert"), None),
        P(),
        P(None, "expert"),
        P(None, "expert"),
        P("expert", None),
    )
    return jax.shard_map(
        shards, mesh=mesh, in_specs=placed, out_specs=P(("dp", "expert"), None), check_vma=False
    )
```

```python
import functools

import jax
import jax.numpy as jnp
from jax import lax
from jax.experimental import pallas as pl
from jax.experimental.pallas import tpu as pltpu
from jax.sharding import PartitionSpec as P

MESH = pl.DeviceIdType.MESH
epsilon = 1e-05
SIDE = 4
BLOCKS = 16
PACK = 4
CHUNK = 16
RING = 8
OFFSETS = (
    (0, 0), (1, 1), (3, 3), (1, 3),
    (3, 1), (2, 0), (0, 2), (1, 0),
    (3, 0), (0, 1), (0, 3), (2, 1),
    (2, 3), (1, 2), (3, 2), (2, 2),
)
OWN = 11
HOSTS = OFFSETS[:OWN] + tuple(((dx + 2) % SIDE, (dy + 2) % SIDE) for dx, dy in OFFSETS[OWN:])
REMOTE = range(1, BLOCKS - 1)
FFN_GROUPS = ((0, 4), (4, 8), (8, 11), (11, 16))
UPWARD = (4, 3, 4)


def kernel(
    cap, ids_ref, weights_ref, modality_ref, gain_ref, tokens_hbm, gate_hbm, up_hbm, down_hbm, out_ref,
    tokens, normed, cols, slots, send, recv, res, ret, own_gate, own_up, own_down,
    far_gate, far_up, far_down, act, acc,
    load_sem, send_sem, recv_sem, back_sem, ret_sem,
    pair_send, pair_recv, ring_send, ring_recv, core_send, core_recv,
):
    rows, width = tokens.shape
    hidden = own_down.shape[0]
    tiles = hidden // 128
    me = lax.axis_index("expert")
    ex, ey = me % SIDE, me // SIDE
    dp = lax.axis_index("dp")
    z, core = dp // 2, dp % 2

    def at_offset(offset, sign):
        dx, dy = offset
        return ((ey + sign * dy + SIDE) % SIDE) * SIDE + (ex + sign * dx + SIDE) % SIDE

    def peer(i, sign):
        return at_offset(HOSTS[i], sign)

    pair = at_offset((2, 2), 1)
    other = z * 2 + 1 - core

    def level(s):
        return (z + s + RING) % RING

    barrier = pltpu.get_barrier_semaphore()
    for i in range(1, OWN):
        pl.semaphore_signal(barrier, inc=1, device_id={"expert": peer(i, 1)}, device_id_type=MESH)
    pl.semaphore_signal(barrier, inc=1, device_id={"expert": pair}, device_id_type=MESH)
    for s in (1, -1):
        pl.semaphore_signal(barrier, inc=1, device_id={"dp": level(s) * 2 + core}, device_id_type=MESH)
    pl.semaphore_signal(barrier, inc=1, device_id={"dp": other}, device_id_type=MESH)

    load = pltpu.make_async_copy(tokens_hbm, tokens, load_sem.at[0])
    load.start()
    loads = [
        pltpu.make_async_copy(gate_hbm, own_gate, load_sem.at[1]),
        pltpu.make_async_copy(up_hbm, own_up, load_sem.at[2]),
        pltpu.make_async_copy(down_hbm, own_down, load_sem.at[3]),
    ]

    def piece(j, k):
        if j == 2:
            return far_down.at[k]
        return (far_gate, far_up)[j].at[pl.ds(pl.multiple_of(k * 128, 128), 128), :]

    def source_piece(j):
        at = pl.ds(pl.multiple_of(dp * 128, 128), 128)
        return (gate_hbm.at[at, :], up_hbm.at[at, :], down_hbm.at[:, at])[j]

    def pair_copy(j):
        return pltpu.make_async_remote_copy(
            src_ref=source_piece(j), dst_ref=piece(j, dp), send_sem=pair_send.at[j], recv_sem=pair_recv.at[j],
            device_id={"expert": pair}, device_id_type=MESH,
        )

    def ring_copy(j, up, s, origin):
        n = (j * 2 + (0 if up else 1)) * 4 + s - 1
        k = origin * 2 + core
        return pltpu.make_async_remote_copy(
            src_ref=piece(j, k), dst_ref=piece(j, k), send_sem=ring_send.at[n], recv_sem=ring_recv.at[n],
            device_id={"dp": level(1 if up else -1) * 2 + core}, device_id_type=MESH,
        )

    def core_copy(j, n, k):
        return pltpu.make_async_remote_copy(
            src_ref=piece(j, k), dst_ref=piece(j, k), send_sem=core_send.at[j * RING + n],
            recv_sem=core_recv.at[j * RING + n], device_id={"dp": other}, device_id_type=MESH,
        )

    def limit(j, up):
        return UPWARD[j] if up else RING - 1 - UPWARD[j]

    def place(up, s):
        return 0 if s == 0 else (s if up else 4 + s)

    core_slots = {}
    for j in range(3):
        found = [(0, 0)] + [(s, -s) for s in range(1, limit(j, True) + 1)]
        found += [(limit(j, True) + s, s) for s in range(1, limit(j, False) + 1)]
        core_slots[j] = found
    sent = []

    def forward(j, up, s):
        if s == 0:
            pair_copy(j).wait_recv()
            n, origin = 0, level(0)
            for way in (True, False):
                copy = ring_copy(j, way, 1, origin)
                copy.start()
                sent.append(copy)
        else:
            origin = level(-s if up else s)
            ring_copy(j, up, s, origin).wait_recv()
            n = s if up else limit(j, True) + s
            if s < limit(j, up):
                copy = ring_copy(j, up, s + 1, origin)
                copy.start()
                sent.append(copy)
        copy = core_copy(j, n, origin * 2 + core)
        copy.start()
        sent.append(copy)

    events = [(j, True, 0) for j in range(3)]
    for s in range(1, 5):
        for j in range(3):
            events += [(j, up, s) for up in (True, False) if s <= limit(j, up)]
    pending = iter(events)

    def advance(count):
        for _ in range(count):
            event = next(pending, None)
            if event is not None:
                forward(*event)

    pl.semaphore_wait(barrier, OWN + 3)
    for j in range(3):
        pair_copy(j).start()
    for copy in loads:
        copy.start()

    id0, id1 = ids_ref[0:1, :], ids_ref[1:2, :]
    w0, w1 = weights_ref[0:1, :], weights_ref[1:2, :]
    experts = lax.broadcasted_iota(jnp.int32, (BLOCKS, rows), 0)
    is0, is1 = experts == id0, experts == id1
    names = jnp.where(is0 | is1, 1.0, 0.0).astype(jnp.bfloat16)
    before = lax.broadcasted_iota(jnp.int32, (rows, rows), 0) < lax.broadcasted_iota(jnp.int32, (rows, rows), 1)
    earlier = jnp.dot(names, jnp.where(before, 1.0, 0.0).astype(jnp.bfloat16), preferred_element_type=jnp.float32)
    pos0 = jnp.sum(jnp.where(is0, earlier, 0.0), axis=0, keepdims=True)
    pos1 = jnp.sum(jnp.where(is1, earlier, 0.0), axis=0, keepdims=True)
    base0, base1 = jnp.zeros_like(pos0), jnp.zeros_like(pos1)
    for i in range(1, BLOCKS):
        name = at_offset(OFFSETS[i], 1)
        base0 = jnp.where(id0 == name, float(i * cap), base0)
        base1 = jnp.where(id1 == name, float(i * cap), base1)
    slot0, slot1 = base0 + pos0, base1 + pos1
    hi0, hi1 = w0.astype(jnp.bfloat16).astype(jnp.float32), w1.astype(jnp.bfloat16).astype(jnp.float32)
    slots[0:1, :] = slot0.astype(jnp.int32)
    slots[1:2, :] = slot1.astype(jnp.int32)
    kind = modality_ref[...].astype(jnp.float32)
    table = jnp.concatenate([slot0, slot1, hi0, hi1, w0 - hi0, w1 - hi1, kind, jnp.zeros_like(kind)], axis=0)
    cols[...] = jnp.concatenate([table, jnp.zeros((120, rows), jnp.float32)], axis=0).T

    load.wait()
    step = 64

    def norm_step(r, carry):
        at = pl.ds(pl.multiple_of(r * step, step), step)
        values = tokens[at, :].astype(jnp.float32)
        square = jnp.mean(values * values, axis=1, keepdims=True)
        gains = jnp.where(cols[at, 6:7] == 1.0, gain_ref[1:2, :], gain_ref[0:1, :])
        normed[at, :] = (values * lax.rsqrt(square + epsilon) * gains).astype(jnp.bfloat16)
        return carry

    lax.fori_loop(0, rows // step, norm_step, 0)

    def parts(source, target, sems, rsems, i, device):
        return [
            pltpu.make_async_remote_copy(
                src_ref=source.at[i, pl.ds(c * CHUNK, CHUNK), :],
                dst_ref=target.at[i, pl.ds(c * CHUNK, CHUNK), :],
                send_sem=sems.at[i],
                recv_sem=rsems.at[i],
                device_id={"expert": device},
                device_id_type=MESH,
            )
            for c in range(cap // CHUNK)
        ]

    def whole(source, target, sems, rsems, i, device):
        return pltpu.make_async_remote_copy(
            src_ref=source.at[i],
            dst_ref=target.at[i],
            send_sem=sems.at[i],
            recv_sem=rsems.at[i],
            device_id={"expert": device},
            device_id_type=MESH,
        )

    def start_all(source, target, sems, rsems, blocks, sign):
        lists = [parts(source, target, sems, rsems, i, peer(i, sign)) for i in blocks]
        for c in range(cap // CHUNK):
            for copies in lists:
                copies[c].start()

    def store(first, last, values, at, remote, local):
        values = values.reshape(last - first, cap, values.shape[-1])
        low, high = max(first, 1), min(last, BLOCKS - 1)
        if first < low:
            local[0:1, :, at] = values[0:1]
        if last > high:
            local[high:last, :, at] = values[high - first :]
        remote[low:high, :, at] = values[low - first : high - first]

    def pack(first, last):
        span = (last - first) * cap
        places = lax.broadcasted_iota(jnp.int32, (span, rows), 0) + first * cap
        pick = jnp.where((places == slots[0:1, :]) | (places == slots[1:2, :]), 1.0, 0.0).astype(jnp.bfloat16)
        part = width // 4

        def pack_step(n, carry):
            at = pl.ds(pl.multiple_of(n * part, part), part)
            packed = jnp.dot(pick, normed[:, at], preferred_element_type=jnp.float32).astype(jnp.bfloat16)
            store(first, last, packed, at, send, recv)
            return carry

        lax.fori_loop(0, 4, pack_step, 0)
        start_all(send, recv, send_sem, recv_sem, [i for i in range(first, last) if i in REMOTE], 1)

    def wait_blocks(first, last, returning):
        for i in range(first, last):
            if i in REMOTE:
                if returning:
                    whole(res, ret, back_sem, ret_sem, i, peer(i, -1)).wait_recv()
                else:
                    whole(send, recv, send_sem, recv_sem, i, peer(i, 1)).wait_recv()

    def ffn_hidden(first, last, gate_w, up_w):
        span = (last - first) * cap

        def hidden_step(t, carry):
            at = pl.ds(pl.multiple_of(t * 128, 128), 128)
            flat = recv[first:last].reshape(span, width)
            weights = jnp.concatenate([gate_w[:, at], up_w[:, at]], axis=1)
            both = jnp.dot(flat, weights, preferred_element_type=jnp.float32)
            gate, upper = both[:, :128], both[:, 128:]
            act[0:span, at] = (jax.nn.silu(gate) * upper).astype(jnp.bfloat16)
            return carry

        lax.fori_loop(0, tiles, hidden_step, 0)

    def ffn_down(first, last, down_w):
        span = (last - first) * cap

        def down_step(n, carry):
            at = pl.ds(pl.multiple_of(n * 256, 256), 256)
            done = jnp.dot(act[0:span, :], down_w(n, at), preferred_element_type=jnp.float32)
            store(first, last, done.astype(jnp.bfloat16), at, res, ret)
            return carry

        lax.fori_loop(0, width // 256, down_step, 0)
        start_all(res, ret, back_sem, ret_sem, [i for i in range(first, last) if i in REMOTE], -1)

    def mix(first, last, begin, end):
        span = (last - first) * cap
        places = (lax.broadcasted_iota(jnp.int32, (rows, span), 1) + first * cap).astype(jnp.float32)
        at0, at1 = places == cols[:, 0:1], places == cols[:, 1:2]
        high = (jnp.where(at0, cols[:, 2:3], 0.0) + jnp.where(at1, cols[:, 3:4], 0.0)).astype(jnp.bfloat16)
        low = (jnp.where(at0, cols[:, 4:5], 0.0) + jnp.where(at1, cols[:, 5:6], 0.0)).astype(jnp.bfloat16)

        def mix_step(n, carry):
            at = pl.ds(pl.multiple_of(n * 256, 256), 256)
            block = ret[first:last, :, at].reshape(span, 256)
            total = jnp.dot(high, block, preferred_element_type=jnp.float32)
            total = total + jnp.dot(low, block, preferred_element_type=jnp.float32)
            if not begin:
                total = total + acc[:, at]
            if end:
                out_ref[:, at] = (tokens[:, at].astype(jnp.float32) + total).astype(jnp.bfloat16)
            else:
                acc[:, at] = total
            return carry

        lax.fori_loop(0, width // 256, mix_step, 0)

    pack(0, 4)
    advance(1)
    pack(4, 8)
    advance(1)
    pack(8, 12)
    advance(1)
    pack(12, 16)

    for copy in loads:
        copy.wait()
    own_columns = lambda n, at: own_down[:, at]
    for first, last in FFN_GROUPS[:3]:
        wait_blocks(first, last, False)
        ffn_hidden(first, last, own_gate, own_up)
        advance(2)
        ffn_down(first, last, own_columns)
        advance(2)
    advance(2)
    wait_blocks(0, 4, True)
    mix(0, 4, True, False)
    advance(len(events))

    for j in range(3):
        for n, origin in core_slots[j]:
            core_copy(j, n, level(origin) * 2 + 1 - core).wait_recv()
    far_columns = lambda n, at: jnp.concatenate([far_down[2 * n], far_down[2 * n + 1]], axis=1)
    wait_blocks(11, 16, False)
    ffn_hidden(11, 16, far_gate, far_up)
    ffn_down(11, 16, far_columns)
    wait_blocks(4, 8, True)
    mix(4, 8, False, False)
    wait_blocks(8, 11, True)
    mix(8, 11, False, False)
    wait_blocks(11, 16, True)
    mix(11, 16, False, True)

    for i in REMOTE:
        whole(send, recv, send_sem, recv_sem, i, peer(i, 1)).wait_send()
        whole(res, ret, back_sem, ret_sem, i, peer(i, -1)).wait_send()
    for j in range(3):
        pair_copy(j).wait_send()
    for copy in sent:
        copy.wait_send()


def shards(tokens, modality, expert_ids, route_weights, norm_gain, gate_weight, up_weight, down_weight):
    rows, width = tokens.shape
    fanout = expert_ids.shape[1]
    hidden = down_weight.shape[0]
    cap = min(rows, rows * fanout * 5 // (4 * BLOCKS))
    anywhere = pl.BlockSpec(memory_space=pl.ANY)
    vmem = pl.BlockSpec(memory_space=pltpu.VMEM)
    block = pltpu.VMEM((BLOCKS, cap, width), jnp.bfloat16)
    sems = pltpu.SemaphoreType.DMA((BLOCKS,))
    dma = pltpu.SemaphoreType.DMA
    longest = max(last - first for first, last in FFN_GROUPS)
    return pl.pallas_call(
        functools.partial(kernel, cap),
        out_shape=jax.ShapeDtypeStruct((rows, width), jnp.bfloat16),
        in_specs=[vmem, vmem, vmem, vmem, anywhere, anywhere, anywhere, anywhere],
        out_specs=vmem,
        scratch_shapes=[
            pltpu.VMEM((rows, width), jnp.bfloat16),
            pltpu.VMEM((rows, width), jnp.bfloat16),
            pltpu.VMEM((rows, 128), jnp.float32),
            pltpu.VMEM((8, rows), jnp.int32),
            block, block, block, block,
            pltpu.VMEM((width, hidden), jnp.bfloat16),
            pltpu.VMEM((width, hidden), jnp.bfloat16),
            pltpu.VMEM((hidden, width), jnp.bfloat16),
            pltpu.VMEM((width, hidden), jnp.bfloat16),
            pltpu.VMEM((width, hidden), jnp.bfloat16),
            pltpu.VMEM((width // 128, hidden, 128), jnp.bfloat16),
            pltpu.VMEM((longest * cap, hidden), jnp.bfloat16),
            pltpu.VMEM((rows, width), jnp.float32),
            dma((4,)),
            sems, sems, sems, sems,
            dma((3,)), dma((3,)), dma((24,)), dma((24,)), dma((24,)), dma((24,)),
        ],
        compiler_params=pltpu.CompilerParams(
            collective_id=0, has_side_effects=True, vmem_limit_bytes=63 * 1024 * 1024
        ),
    )(expert_ids.T, route_weights.T, modality[None, :], norm_gain, tokens, gate_weight, up_weight, down_weight)


def solution(mesh):
    placed = (
        P(("dp", "expert"), None),
        P(("dp", "expert")),
        P(("dp", "expert"), None),
        P(("dp", "expert"), None),
        P(),
        P(None, "expert"),
        P(None, "expert"),
        P("expert", None),
    )
    return jax.shard_map(
        shards, mesh=mesh, in_specs=placed, out_specs=P(("dp", "expert"), None), check_vma=False
    )
```

```python
import functools

import jax
import jax.numpy as jnp
from jax import lax
from jax.experimental import pallas as pl
from jax.experimental.pallas import tpu as pltpu
from jax.sharding import PartitionSpec as P

MESH = pl.DeviceIdType.MESH
epsilon = 1e-05
SIDE = 4
BLOCKS = 16
PACK = 4
RING = 8
OFFSETS = (
    (0, 0), (1, 1), (3, 3), (1, 3),
    (3, 1), (2, 0), (0, 2), (1, 0),
    (3, 0), (0, 1), (0, 3), (2, 1),
    (2, 3), (1, 2), (3, 2), (2, 2),
)
OWN = 11
HOSTS = OFFSETS[:OWN] + tuple(((dx + 2) % SIDE, (dy + 2) % SIDE) for dx, dy in OFFSETS[OWN:])
REMOTE = range(1, BLOCKS - 1)
FFN_GROUPS = ((0, 4), (4, 8), (8, 11), (11, 16))
UPWARD = (4, 3, 4)


def kernel(
    cap, ids_ref, weights_ref, modality_ref, gain_ref, tokens_hbm, gate_hbm, up_hbm, down_hbm, out_ref,
    tokens, normed, cols, slots, send, recv, res, ret, own_gate, own_up, own_down,
    far_gate, far_up, far_down, act, acc, picks, own_mix, far_mix,
    load_sem, send_sem, recv_sem, back_sem, ret_sem,
    pair_send, pair_recv, ring_send, ring_recv, core_send, core_recv,
):
    rows, width = tokens.shape
    hidden = own_down.shape[0]
    tiles = hidden // 128
    me = lax.axis_index("expert")
    ex, ey = me % SIDE, me // SIDE
    dp = lax.axis_index("dp")
    z, core = dp // 2, dp % 2

    def at_offset(offset, sign):
        dx, dy = offset
        return ((ey + sign * dy + SIDE) % SIDE) * SIDE + (ex + sign * dx + SIDE) % SIDE

    def peer(i, sign):
        return at_offset(HOSTS[i], sign)

    pair = at_offset((2, 2), 1)
    other = z * 2 + 1 - core

    def level(s):
        return (z + s + RING) % RING

    barrier = pltpu.get_barrier_semaphore()
    for i in range(1, OWN):
        pl.semaphore_signal(barrier, inc=1, device_id={"expert": peer(i, 1)}, device_id_type=MESH)
    pl.semaphore_signal(barrier, inc=1, device_id={"expert": pair}, device_id_type=MESH)
    for s in (1, -1):
        pl.semaphore_signal(barrier, inc=1, device_id={"dp": level(s) * 2 + core}, device_id_type=MESH)
    pl.semaphore_signal(barrier, inc=1, device_id={"dp": other}, device_id_type=MESH)

    load = pltpu.make_async_copy(tokens_hbm, tokens, load_sem.at[0])
    load.start()
    loads = [
        pltpu.make_async_copy(gate_hbm, own_gate, load_sem.at[1]),
        pltpu.make_async_copy(up_hbm, own_up, load_sem.at[2]),
        pltpu.make_async_copy(down_hbm, own_down, load_sem.at[3]),
    ]

    def piece(j, k):
        if j == 2:
            return far_down.at[k]
        return (far_gate, far_up)[j].at[pl.ds(pl.multiple_of(k * 128, 128), 128), :]

    def source_piece(j):
        at = pl.ds(pl.multiple_of(dp * 128, 128), 128)
        return (gate_hbm.at[at, :], up_hbm.at[at, :], down_hbm.at[:, at])[j]

    def pair_copy(j):
        return pltpu.make_async_remote_copy(
            src_ref=source_piece(j), dst_ref=piece(j, dp), send_sem=pair_send.at[j], recv_sem=pair_recv.at[j],
            device_id={"expert": pair}, device_id_type=MESH,
        )

    def ring_copy(j, up, s, origin):
        n = (j * 2 + (0 if up else 1)) * 4 + s - 1
        k = origin * 2 + core
        return pltpu.make_async_remote_copy(
            src_ref=piece(j, k), dst_ref=piece(j, k), send_sem=ring_send.at[n], recv_sem=ring_recv.at[n],
            device_id={"dp": level(1 if up else -1) * 2 + core}, device_id_type=MESH,
        )

    def core_copy(j, n, k):
        return pltpu.make_async_remote_copy(
            src_ref=piece(j, k), dst_ref=piece(j, k), send_sem=core_send.at[j * RING + n],
            recv_sem=core_recv.at[j * RING + n], device_id={"dp": other}, device_id_type=MESH,
        )

    def limit(j, up):
        return UPWARD[j] if up else RING - 1 - UPWARD[j]

    def place(up, s):
        return 0 if s == 0 else (s if up else 4 + s)

    core_slots = {}
    for j in range(3):
        found = [(0, 0)] + [(s, -s) for s in range(1, limit(j, True) + 1)]
        found += [(limit(j, True) + s, s) for s in range(1, limit(j, False) + 1)]
        core_slots[j] = found
    sent = []

    def forward(j, up, s):
        if s == 0:
            pair_copy(j).wait_recv()
            n, origin = 0, level(0)
            for way in (True, False):
                copy = ring_copy(j, way, 1, origin)
                copy.start()
                sent.append(copy)
        else:
            origin = level(-s if up else s)
            ring_copy(j, up, s, origin).wait_recv()
            n = s if up else limit(j, True) + s
            if s < limit(j, up):
                copy = ring_copy(j, up, s + 1, origin)
                copy.start()
                sent.append(copy)
        copy = core_copy(j, n, origin * 2 + core)
        copy.start()
        sent.append(copy)

    events = [(j, True, 0) for j in range(3)]
    for s in range(1, 5):
        for j in range(3):
            events += [(j, up, s) for up in (True, False) if s <= limit(j, up)]
    pending = iter(events)

    def advance(count):
        for _ in range(count):
            event = next(pending, None)
            if event is not None:
                forward(*event)

    pl.semaphore_wait(barrier, OWN + 3)
    for j in range(3):
        pair_copy(j).start()
    for copy in loads:
        copy.start()

    id0, id1 = ids_ref[0:1, :], ids_ref[1:2, :]
    w0, w1 = weights_ref[0:1, :], weights_ref[1:2, :]
    experts = lax.broadcasted_iota(jnp.int32, (BLOCKS, rows), 0)
    is0, is1 = experts == id0, experts == id1
    names = jnp.where(is0 | is1, 1.0, 0.0).astype(jnp.bfloat16)
    before = lax.broadcasted_iota(jnp.int32, (rows, rows), 0) < lax.broadcasted_iota(jnp.int32, (rows, rows), 1)
    earlier = jnp.dot(names, jnp.where(before, 1.0, 0.0).astype(jnp.bfloat16), preferred_element_type=jnp.float32)
    pos0 = jnp.sum(jnp.where(is0, earlier, 0.0), axis=0, keepdims=True)
    pos1 = jnp.sum(jnp.where(is1, earlier, 0.0), axis=0, keepdims=True)
    base0, base1 = jnp.zeros_like(pos0), jnp.zeros_like(pos1)
    for i in range(1, BLOCKS):
        name = at_offset(OFFSETS[i], 1)
        base0 = jnp.where(id0 == name, float(i * cap), base0)
        base1 = jnp.where(id1 == name, float(i * cap), base1)
    slot0, slot1 = base0 + pos0, base1 + pos1
    slots[0:1, :] = slot0.astype(jnp.int32)
    slots[1:2, :] = slot1.astype(jnp.int32)
    kind = modality_ref[...].astype(jnp.float32)
    table = jnp.concatenate([slot0, slot1, w0, w1, kind, kind, kind, kind], axis=0)
    cols[...] = jnp.concatenate([table, jnp.zeros((120, rows), jnp.float32)], axis=0).T

    load.wait()
    step = 64

    def norm_step(r, carry):
        at = pl.ds(pl.multiple_of(r * step, step), step)
        values = tokens[at, :].astype(jnp.float32)
        square = jnp.mean(values * values, axis=1, keepdims=True)
        gains = jnp.where(cols[at, 4:5] == 1.0, gain_ref[1:2, :], gain_ref[0:1, :])
        normed[at, :] = (values * lax.rsqrt(square + epsilon) * gains).astype(jnp.bfloat16)
        return carry

    lax.fori_loop(0, rows // step, norm_step, 0)

    def whole(source, target, sems, rsems, i, device):
        return pltpu.make_async_remote_copy(
            src_ref=source.at[i],
            dst_ref=target.at[i],
            send_sem=sems.at[i],
            recv_sem=rsems.at[i],
            device_id={"expert": device},
            device_id_type=MESH,
        )

    def start_all(source, target, sems, rsems, blocks, sign):
        for i in blocks:
            whole(source, target, sems, rsems, i, peer(i, sign)).start()

    def store(first, last, values, at, remote, local):
        values = values.reshape(last - first, cap, values.shape[-1])
        low, high = max(first, 1), min(last, BLOCKS - 1)
        if first < low:
            local[0:1, :, at] = values[0:1]
        if last > high:
            local[high:last, :, at] = values[high - first :]
        remote[low:high, :, at] = values[low - first : high - first]

    def pack(first, last):
        span = (last - first) * cap
        part = width // 4

        def pick_step(n, carry):
            places = lax.broadcasted_iota(jnp.int32, (cap, rows), 0) + (first + n) * cap
            found = (places == slots[0:1, :]) | (places == slots[1:2, :])
            picks[pl.ds(pl.multiple_of(n * cap, cap), cap), :] = jnp.where(found, 1.0, 0.0).astype(jnp.bfloat16)
            return carry

        lax.fori_loop(0, last - first, pick_step, 0)

        def pack_step(n, carry):
            at = pl.ds(pl.multiple_of(n * part, part), part)
            packed = jnp.dot(picks[0:span, :], normed[:, at], preferred_element_type=jnp.float32).astype(jnp.bfloat16)
            store(first, last, packed, at, send, recv)
            return carry

        lax.fori_loop(0, 4, pack_step, 0)
        start_all(send, recv, send_sem, recv_sem, [i for i in range(first, last) if i in REMOTE], 1)

    def wait_blocks(first, last, returning):
        for i in range(first, last):
            if i in REMOTE:
                if returning:
                    whole(res, ret, back_sem, ret_sem, i, peer(i, -1)).wait_recv()
                else:
                    whole(send, recv, send_sem, recv_sem, i, peer(i, 1)).wait_recv()

    def ffn_hidden(first, last, gate_w, up_w):
        span = (last - first) * cap

        def hidden_step(t, carry):
            at = pl.ds(pl.multiple_of(t * 128, 128), 128)
            flat = recv[first:last].reshape(span, width)
            weights = jnp.concatenate([gate_w[:, at], up_w[:, at]], axis=1)
            both = jnp.dot(flat, weights, preferred_element_type=jnp.float32)
            gate, upper = both[:, :128], both[:, 128:]
            act[0:span, at] = (jax.nn.silu(gate) * upper).astype(jnp.bfloat16)
            return carry

        lax.fori_loop(0, tiles, hidden_step, 0)

    def ffn_down(first, last, down_w):
        span = (last - first) * cap

        def down_step(n, carry):
            at = pl.ds(pl.multiple_of(n * 256, 256), 256)
            done = jnp.dot(act[0:span, :], down_w(n, at), preferred_element_type=jnp.float32)
            store(first, last, done.astype(jnp.bfloat16), at, res, ret)
            return carry

        lax.fori_loop(0, width // 256, down_step, 0)
        start_all(res, ret, back_sem, ret_sem, [i for i in range(first, last) if i in REMOTE], -1)

    def mix_table(first, last, table):
        span = (last - first) * cap

        def table_step(r, carry):
            at = pl.ds(pl.multiple_of(r * step, step), step)
            places = (lax.broadcasted_iota(jnp.int32, (step, span), 1) + first * cap).astype(jnp.float32)
            first_choice = jnp.where(places == cols[at, 0:1], cols[at, 2:3], 0.0)
            second_choice = jnp.where(places == cols[at, 1:2], cols[at, 3:4], 0.0)
            table[at, :] = (first_choice + second_choice).astype(jnp.bfloat16)
            return carry

        lax.fori_loop(0, rows // step, table_step, 0)

    def mix(first, last, table, end):
        span = (last - first) * cap

        def mix_step(n, carry):
            at = pl.ds(pl.multiple_of(n * 256, 256), 256)
            block = ret[first:last, :, at].reshape(span, 256)
            total = jnp.dot(table[...], block, preferred_element_type=jnp.float32)
            if end:
                out_ref[:, at] = (acc[:, at] + total).astype(jnp.bfloat16)
            else:
                acc[:, at] = tokens[:, at].astype(jnp.float32) + total
            return carry

        lax.fori_loop(0, width // 256, mix_step, 0)

    def core_wait(j):
        for n, origin in core_slots[j]:
            core_copy(j, n, level(origin) * 2 + 1 - core).wait_recv()

    own_columns = lambda n, at: own_down[:, at]
    far_columns = lambda n, at: jnp.concatenate([far_down[2 * n], far_down[2 * n + 1]], axis=1)

    pack(0, 4)
    advance(1)
    pack(4, 8)
    advance(1)
    pack(8, 12)
    advance(1)
    pack(12, 16)
    advance(2)
    mix_table(0, OWN, own_mix)
    mix_table(OWN, BLOCKS, far_mix)
    for copy in loads:
        copy.wait()
    advance(2)
    wait_blocks(0, 4, False)
    ffn_hidden(0, 4, own_gate, own_up)
    advance(2)
    ffn_down(0, 4, own_columns)
    advance(4)
    wait_blocks(4, 8, False)
    ffn_hidden(4, 8, own_gate, own_up)
    advance(2)
    ffn_down(4, 8, own_columns)
    advance(4)
    wait_blocks(8, OWN, False)
    ffn_hidden(8, OWN, own_gate, own_up)
    advance(2)
    ffn_down(8, OWN, own_columns)
    advance(2)
    core_wait(0)
    core_wait(1)
    wait_blocks(OWN, BLOCKS, False)
    ffn_hidden(OWN, BLOCKS, far_gate, far_up)
    advance(1)
    core_wait(2)
    ffn_down(OWN, BLOCKS, far_columns)
    wait_blocks(0, OWN, True)
    mix(0, OWN, own_mix, False)
    wait_blocks(OWN, BLOCKS, True)
    mix(OWN, BLOCKS, far_mix, True)

    for i in REMOTE:
        whole(send, recv, send_sem, recv_sem, i, peer(i, 1)).wait_send()
        whole(res, ret, back_sem, ret_sem, i, peer(i, -1)).wait_send()
    for j in range(3):
        pair_copy(j).wait_send()
    for copy in sent:
        copy.wait_send()


def shards(tokens, modality, expert_ids, route_weights, norm_gain, gate_weight, up_weight, down_weight):
    rows, width = tokens.shape
    fanout = expert_ids.shape[1]
    hidden = down_weight.shape[0]
    cap = min(rows, rows * fanout * 5 // (4 * BLOCKS))
    anywhere = pl.BlockSpec(memory_space=pl.ANY)
    vmem = pl.BlockSpec(memory_space=pltpu.VMEM)
    block = pltpu.VMEM((BLOCKS, cap, width), jnp.bfloat16)
    sems = pltpu.SemaphoreType.DMA((BLOCKS,))
    dma = pltpu.SemaphoreType.DMA
    longest = max(last - first for first, last in FFN_GROUPS)
    return pl.pallas_call(
        functools.partial(kernel, cap),
        out_shape=jax.ShapeDtypeStruct((rows, width), jnp.bfloat16),
        in_specs=[vmem, vmem, vmem, vmem, anywhere, anywhere, anywhere, anywhere],
        out_specs=vmem,
        scratch_shapes=[
            pltpu.VMEM((rows, width), jnp.bfloat16),
            pltpu.VMEM((rows, width), jnp.bfloat16),
            pltpu.VMEM((rows, 128), jnp.float32),
            pltpu.VMEM((8, rows), jnp.int32),
            block, block, block, block,
            pltpu.VMEM((width, hidden), jnp.bfloat16),
            pltpu.VMEM((width, hidden), jnp.bfloat16),
            pltpu.VMEM((hidden, width), jnp.bfloat16),
            pltpu.VMEM((width, hidden), jnp.bfloat16),
            pltpu.VMEM((width, hidden), jnp.bfloat16),
            pltpu.VMEM((width // 128, hidden, 128), jnp.bfloat16),
            pltpu.VMEM((longest * cap, hidden), jnp.bfloat16),
            pltpu.VMEM((rows, width), jnp.float32),
            pltpu.VMEM((PACK * cap, rows), jnp.bfloat16),
            pltpu.VMEM((rows, OWN * cap), jnp.bfloat16),
            pltpu.VMEM((rows, (BLOCKS - OWN) * cap), jnp.bfloat16),
            dma((4,)),
            sems, sems, sems, sems,
            dma((3,)), dma((3,)), dma((24,)), dma((24,)), dma((24,)), dma((24,)),
        ],
        compiler_params=pltpu.CompilerParams(
            collective_id=0, has_side_effects=True, vmem_limit_bytes=63 * 1024 * 1024
        ),
    )(expert_ids.T, route_weights.T, modality[None, :], norm_gain, tokens, gate_weight, up_weight, down_weight)


def solution(mesh):
    placed = (
        P(("dp", "expert"), None),
        P(("dp", "expert")),
        P(("dp", "expert"), None),
        P(("dp", "expert"), None),
        P(),
        P(None, "expert"),
        P(None, "expert"),
        P("expert", None),
    )
    return jax.shard_map(
        shards, mesh=mesh, in_specs=placed, out_specs=P(("dp", "expert"), None), check_vma=False
    )
```

```python
import functools

import jax
import jax.numpy as jnp
from jax import lax
from jax.experimental import pallas as pl
from jax.experimental.pallas import tpu as pltpu
from jax.sharding import PartitionSpec as P

MESH = pl.DeviceIdType.MESH
epsilon = 1e-05
SIDE = 4
BLOCKS = 16
PACK = 4
RING = 8
OFFSETS = (
    (0, 0), (1, 1), (3, 3), (1, 3),
    (3, 1), (2, 0), (0, 2), (1, 0),
    (3, 0), (0, 1), (0, 3), (2, 1),
    (2, 3), (1, 2), (3, 2), (2, 2),
)
OWN = 11
HOSTS = OFFSETS[:OWN] + tuple(((dx + 2) % SIDE, (dy + 2) % SIDE) for dx, dy in OFFSETS[OWN:])
REMOTE = range(1, BLOCKS - 1)
FFN_GROUPS = ((0, 4), (4, 8), (8, 11), (11, 16))
UPWARD = (4, 3, 4)


def kernel(
    cap, ids_ref, weights_ref, modality_ref, gain_ref, tokens_hbm, gate_hbm, up_hbm, down_hbm, out_hbm,
    tokens, normed, cols, slots, send, recv, res, ret, own_gate, own_up, own_down,
    far_gate, far_up, far_down, act, acc, picks, own_mix, far_mix,
    mixed, load_sem, out_sem, send_sem, recv_sem, back_sem, ret_sem,
    pair_send, pair_recv, ring_send, ring_recv, core_send, core_recv,
):
    rows, width = tokens.shape
    hidden = own_down.shape[0]
    tiles = hidden // 128
    me = lax.axis_index("expert")
    ex, ey = me % SIDE, me // SIDE
    dp = lax.axis_index("dp")
    z, core = dp // 2, dp % 2

    def at_offset(offset, sign):
        dx, dy = offset
        return ((ey + sign * dy + SIDE) % SIDE) * SIDE + (ex + sign * dx + SIDE) % SIDE

    def peer(i, sign):
        return at_offset(HOSTS[i], sign)

    pair = at_offset((2, 2), 1)
    other = z * 2 + 1 - core

    def level(s):
        return (z + s + RING) % RING

    barrier = pltpu.get_barrier_semaphore()
    for i in range(1, OWN):
        pl.semaphore_signal(barrier, inc=1, device_id={"expert": peer(i, 1)}, device_id_type=MESH)
    pl.semaphore_signal(barrier, inc=1, device_id={"expert": pair}, device_id_type=MESH)
    for s in (1, -1):
        pl.semaphore_signal(barrier, inc=1, device_id={"dp": level(s) * 2 + core}, device_id_type=MESH)
    pl.semaphore_signal(barrier, inc=1, device_id={"dp": other}, device_id_type=MESH)

    load = pltpu.make_async_copy(tokens_hbm, tokens, load_sem.at[0])
    load.start()
    loads = [
        pltpu.make_async_copy(gate_hbm, own_gate, load_sem.at[1]),
        pltpu.make_async_copy(up_hbm, own_up, load_sem.at[2]),
        pltpu.make_async_copy(down_hbm, own_down, load_sem.at[3]),
    ]

    def piece(j, k):
        if j == 2:
            return far_down.at[k]
        return (far_gate, far_up)[j].at[pl.ds(pl.multiple_of(k * 128, 128), 128), :]

    def source_piece(j):
        at = pl.ds(pl.multiple_of(dp * 128, 128), 128)
        return (gate_hbm.at[at, :], up_hbm.at[at, :], down_hbm.at[:, at])[j]

    def pair_copy(j):
        return pltpu.make_async_remote_copy(
            src_ref=source_piece(j), dst_ref=piece(j, dp), send_sem=pair_send.at[j], recv_sem=pair_recv.at[j],
            device_id={"expert": pair}, device_id_type=MESH,
        )

    def ring_copy(j, up, s, origin):
        n = (j * 2 + (0 if up else 1)) * 4 + s - 1
        k = origin * 2 + core
        return pltpu.make_async_remote_copy(
            src_ref=piece(j, k), dst_ref=piece(j, k), send_sem=ring_send.at[n], recv_sem=ring_recv.at[n],
            device_id={"dp": level(1 if up else -1) * 2 + core}, device_id_type=MESH,
        )

    def core_copy(j, n, k):
        return pltpu.make_async_remote_copy(
            src_ref=piece(j, k), dst_ref=piece(j, k), send_sem=core_send.at[j * RING + n],
            recv_sem=core_recv.at[j * RING + n], device_id={"dp": other}, device_id_type=MESH,
        )

    def limit(j, up):
        return UPWARD[j] if up else RING - 1 - UPWARD[j]

    def place(up, s):
        return 0 if s == 0 else (s if up else 4 + s)

    core_slots = {}
    for j in range(3):
        found = [(0, 0)] + [(s, -s) for s in range(1, limit(j, True) + 1)]
        found += [(limit(j, True) + s, s) for s in range(1, limit(j, False) + 1)]
        core_slots[j] = found
    sent = []

    def forward(j, up, s):
        if s == 0:
            pair_copy(j).wait_recv()
            n, origin = 0, level(0)
            for way in (True, False):
                copy = ring_copy(j, way, 1, origin)
                copy.start()
                sent.append(copy)
        else:
            origin = level(-s if up else s)
            ring_copy(j, up, s, origin).wait_recv()
            n = s if up else limit(j, True) + s
            if s < limit(j, up):
                copy = ring_copy(j, up, s + 1, origin)
                copy.start()
                sent.append(copy)
        copy = core_copy(j, n, origin * 2 + core)
        copy.start()
        sent.append(copy)

    events = [(j, True, 0) for j in range(3)]
    for s in range(1, 5):
        for j in range(3):
            events += [(j, up, s) for up in (True, False) if s <= limit(j, up)]
    pending = iter(events)

    def advance(count):
        for _ in range(count):
            event = next(pending, None)
            if event is not None:
                forward(*event)

    pl.semaphore_wait(barrier, OWN + 3)
    for j in range(3):
        pair_copy(j).start()
    for copy in loads:
        copy.start()

    id0, id1 = ids_ref[0:1, :], ids_ref[1:2, :]
    w0, w1 = weights_ref[0:1, :], weights_ref[1:2, :]
    experts = lax.broadcasted_iota(jnp.int32, (BLOCKS, rows), 0)
    is0, is1 = experts == id0, experts == id1
    names = jnp.where(is0 | is1, 1.0, 0.0).astype(jnp.bfloat16)
    before = lax.broadcasted_iota(jnp.int32, (rows, rows), 0) < lax.broadcasted_iota(jnp.int32, (rows, rows), 1)
    earlier = jnp.dot(names, jnp.where(before, 1.0, 0.0).astype(jnp.bfloat16), preferred_element_type=jnp.float32)
    pos0 = jnp.sum(jnp.where(is0, earlier, 0.0), axis=0, keepdims=True)
    pos1 = jnp.sum(jnp.where(is1, earlier, 0.0), axis=0, keepdims=True)
    base0, base1 = jnp.zeros_like(pos0), jnp.zeros_like(pos1)
    for i in range(1, BLOCKS):
        name = at_offset(OFFSETS[i], 1)
        base0 = jnp.where(id0 == name, float(i * cap), base0)
        base1 = jnp.where(id1 == name, float(i * cap), base1)
    slot0, slot1 = base0 + pos0, base1 + pos1
    slots[0:1, :] = slot0.astype(jnp.int32)
    slots[1:2, :] = slot1.astype(jnp.int32)
    kind = modality_ref[...].astype(jnp.float32)
    table = jnp.concatenate([slot0, slot1, w0, w1, kind, kind, kind, kind], axis=0)
    cols[...] = jnp.concatenate([table, jnp.zeros((120, rows), jnp.float32)], axis=0).T

    load.wait()
    step = 64

    def norm_step(r, carry):
        at = pl.ds(pl.multiple_of(r * step, step), step)
        values = tokens[at, :].astype(jnp.float32)
        square = jnp.mean(values * values, axis=1, keepdims=True)
        gains = jnp.where(cols[at, 4:5] == 1.0, gain_ref[1:2, :], gain_ref[0:1, :])
        normed[at, :] = (values * lax.rsqrt(square + epsilon) * gains).astype(jnp.bfloat16)
        return carry

    lax.fori_loop(0, rows // step, norm_step, 0)

    def whole(source, target, sems, rsems, i, device):
        return pltpu.make_async_remote_copy(
            src_ref=source.at[i],
            dst_ref=target.at[i],
            send_sem=sems.at[i],
            recv_sem=rsems.at[i],
            device_id={"expert": device},
            device_id_type=MESH,
        )

    def start_all(source, target, sems, rsems, blocks, sign):
        for i in blocks:
            whole(source, target, sems, rsems, i, peer(i, sign)).start()

    def store(first, last, values, at, remote, local):
        values = values.reshape(last - first, cap, values.shape[-1])
        low, high = max(first, 1), min(last, BLOCKS - 1)
        if first < low:
            local[0:1, :, at] = values[0:1]
        if last > high:
            local[high:last, :, at] = values[high - first :]
        remote[low:high, :, at] = values[low - first : high - first]

    def pack(first, last):
        span = (last - first) * cap
        part = width // 4

        def pick_step(n, carry):
            places = lax.broadcasted_iota(jnp.int32, (cap, rows), 0) + (first + n) * cap
            found = (places == slots[0:1, :]) | (places == slots[1:2, :])
            picks[pl.ds(pl.multiple_of(n * cap, cap), cap), :] = jnp.where(found, 1.0, 0.0).astype(jnp.bfloat16)
            return carry

        lax.fori_loop(0, last - first, pick_step, 0)

        def pack_step(n, carry):
            at = pl.ds(pl.multiple_of(n * part, part), part)
            packed = jnp.dot(picks[0:span, :], normed[:, at], preferred_element_type=jnp.float32).astype(jnp.bfloat16)
            store(first, last, packed, at, send, recv)
            return carry

        lax.fori_loop(0, 4, pack_step, 0)
        start_all(send, recv, send_sem, recv_sem, [i for i in range(first, last) if i in REMOTE], 1)

    def wait_blocks(first, last, returning):
        for i in range(first, last):
            if i in REMOTE:
                if returning:
                    whole(res, ret, back_sem, ret_sem, i, peer(i, -1)).wait_recv()
                else:
                    whole(send, recv, send_sem, recv_sem, i, peer(i, 1)).wait_recv()

    def ffn_hidden(first, last, gate_w, up_w):
        span = (last - first) * cap

        def hidden_step(t, carry):
            at = pl.ds(pl.multiple_of(t * 128, 128), 128)
            flat = recv[first:last].reshape(span, width)
            weights = jnp.concatenate([gate_w[:, at], up_w[:, at]], axis=1)
            both = jnp.dot(flat, weights, preferred_element_type=jnp.float32)
            gate, upper = both[:, :128], both[:, 128:]
            act[0:span, at] = (jax.nn.silu(gate) * upper).astype(jnp.bfloat16)
            return carry

        lax.fori_loop(0, tiles, hidden_step, 0)

    def ffn_down(first, last, down_w):
        span = (last - first) * cap

        def down_step(n, carry):
            at = pl.ds(pl.multiple_of(n * 256, 256), 256)
            done = jnp.dot(act[0:span, :], down_w(n, at), preferred_element_type=jnp.float32)
            store(first, last, done.astype(jnp.bfloat16), at, res, ret)
            return carry

        lax.fori_loop(0, width // 256, down_step, 0)
        start_all(res, ret, back_sem, ret_sem, [i for i in range(first, last) if i in REMOTE], -1)

    def mix_table(first, last, table):
        span = (last - first) * cap

        def table_step(r, carry):
            at = pl.ds(pl.multiple_of(r * step, step), step)
            places = (lax.broadcasted_iota(jnp.int32, (step, span), 1) + first * cap).astype(jnp.float32)
            first_choice = jnp.where(places == cols[at, 0:1], cols[at, 2:3], 0.0)
            second_choice = jnp.where(places == cols[at, 1:2], cols[at, 3:4], 0.0)
            table[at, :] = (first_choice + second_choice).astype(jnp.bfloat16)
            return carry

        lax.fori_loop(0, rows // step, table_step, 0)

    def mix(first, last, table, end):
        span = (last - first) * cap

        def mix_step(n, carry):
            at = pl.ds(pl.multiple_of(n * 256, 256), 256)
            block = ret[first:last, :, at].reshape(span, 256)
            total = jnp.dot(table[...], block, preferred_element_type=jnp.float32)
            if end:
                mixed[:, at] = (acc[:, at] + total).astype(jnp.bfloat16)
                pltpu.make_async_copy(mixed.at[:, at], out_hbm.at[:, at], out_sem.at[n]).start()
            else:
                acc[:, at] = tokens[:, at].astype(jnp.float32) + total
            return carry

        lax.fori_loop(0, width // 256, mix_step, 0)

    def core_wait(j):
        for n, origin in core_slots[j]:
            core_copy(j, n, level(origin) * 2 + 1 - core).wait_recv()

    own_columns = lambda n, at: own_down[:, at]
    far_columns = lambda n, at: jnp.concatenate([far_down[2 * n], far_down[2 * n + 1]], axis=1)

    pack(0, 4)
    advance(1)
    pack(4, 8)
    advance(1)
    pack(8, 12)
    advance(1)
    pack(12, 16)
    advance(2)
    mix_table(0, OWN, own_mix)
    mix_table(OWN, BLOCKS, far_mix)
    for copy in loads:
        copy.wait()
    advance(2)
    wait_blocks(0, 4, False)
    ffn_hidden(0, 4, own_gate, own_up)
    advance(2)
    ffn_down(0, 4, own_columns)
    advance(4)
    wait_blocks(4, 8, False)
    ffn_hidden(4, 8, own_gate, own_up)
    advance(2)
    ffn_down(4, 8, own_columns)
    advance(4)
    wait_blocks(8, OWN, False)
    ffn_hidden(8, OWN, own_gate, own_up)
    advance(2)
    ffn_down(8, OWN, own_columns)
    advance(2)
    core_wait(0)
    core_wait(1)
    wait_blocks(OWN, BLOCKS, False)
    ffn_hidden(OWN, BLOCKS, far_gate, far_up)
    advance(1)
    core_wait(2)
    ffn_down(OWN, BLOCKS, far_columns)
    wait_blocks(0, OWN, True)
    mix(0, OWN, own_mix, False)
    wait_blocks(OWN, BLOCKS, True)
    mix(OWN, BLOCKS, far_mix, True)

    for i in REMOTE:
        whole(send, recv, send_sem, recv_sem, i, peer(i, 1)).wait_send()
        whole(res, ret, back_sem, ret_sem, i, peer(i, -1)).wait_send()
    for j in range(3):
        pair_copy(j).wait_send()
    for copy in sent:
        copy.wait_send()
    for n in range(width // 256):
        at = pl.ds(n * 256, 256)
        pltpu.make_async_copy(mixed.at[:, at], out_hbm.at[:, at], out_sem.at[n]).wait()


def hand_over(source, target, held, in_sem, out_sem):
    count = held.shape[0]
    reads = [pltpu.make_async_copy(source.at[n], held.at[n], in_sem.at[n]) for n in range(count)]
    writes = [pltpu.make_async_copy(held.at[n], target.at[n], out_sem.at[n]) for n in range(count)]
    for read in reads:
        read.start()
    for read, write in zip(reads, writes):
        read.wait()
        write.start()
    for write in writes:
        write.wait()


def shards(tokens, modality, expert_ids, route_weights, norm_gain, gate_weight, up_weight, down_weight):
    rows, width = tokens.shape
    fanout = expert_ids.shape[1]
    hidden = down_weight.shape[0]
    cap = min(rows, rows * fanout * 5 // (4 * BLOCKS))
    anywhere = pl.BlockSpec(memory_space=pl.ANY)
    vmem = pl.BlockSpec(memory_space=pltpu.VMEM)
    block = pltpu.VMEM((BLOCKS, cap, width), jnp.bfloat16)
    sems = pltpu.SemaphoreType.DMA((BLOCKS,))
    dma = pltpu.SemaphoreType.DMA
    longest = max(last - first for first, last in FFN_GROUPS)
    result = pl.pallas_call(
        functools.partial(kernel, cap),
        out_shape=jax.ShapeDtypeStruct((rows, width), jnp.bfloat16),
        in_specs=[vmem, vmem, vmem, vmem, anywhere, anywhere, anywhere, anywhere],
        out_specs=anywhere,
        scratch_shapes=[
            pltpu.VMEM((rows, width), jnp.bfloat16),
            pltpu.VMEM((rows, width), jnp.bfloat16),
            pltpu.VMEM((rows, 128), jnp.float32),
            pltpu.VMEM((8, rows), jnp.int32),
            block, block, block, block,
            pltpu.VMEM((width, hidden), jnp.bfloat16),
            pltpu.VMEM((width, hidden), jnp.bfloat16),
            pltpu.VMEM((hidden, width), jnp.bfloat16),
            pltpu.VMEM((width, hidden), jnp.bfloat16),
            pltpu.VMEM((width, hidden), jnp.bfloat16),
            pltpu.VMEM((width // 128, hidden, 128), jnp.bfloat16),
            pltpu.VMEM((longest * cap, hidden), jnp.bfloat16),
            pltpu.VMEM((rows, width), jnp.float32),
            pltpu.VMEM((PACK * cap, rows), jnp.bfloat16),
            pltpu.VMEM((rows, OWN * cap), jnp.bfloat16),
            pltpu.VMEM((rows, (BLOCKS - OWN) * cap), jnp.bfloat16),
            pltpu.VMEM((rows, width), jnp.bfloat16),
            dma((4,)),
            dma((width // 256,)),
            sems, sems, sems, sems,
            dma((3,)), dma((3,)), dma((24,)), dma((24,)), dma((24,)), dma((24,)),
        ],
        compiler_params=pltpu.CompilerParams(
            collective_id=0, has_side_effects=True, vmem_limit_bytes=63 * 1024 * 1024
        ),
    )(expert_ids.T, route_weights.T, modality[None, :], norm_gain, tokens, gate_weight, up_weight, down_weight)
    pieces = 8
    shape = (pieces, rows // pieces, width)
    return pl.pallas_call(
        hand_over,
        out_shape=jax.ShapeDtypeStruct(shape, jnp.bfloat16),
        in_specs=[anywhere],
        out_specs=anywhere,
        scratch_shapes=[pltpu.VMEM(shape, jnp.bfloat16), dma((pieces,)), dma((pieces,))],
    )(result.reshape(shape)).reshape(rows, width)


def solution(mesh):
    placed = (
        P(("dp", "expert"), None),
        P(("dp", "expert")),
        P(("dp", "expert"), None),
        P(("dp", "expert"), None),
        P(),
        P(None, "expert"),
        P(None, "expert"),
        P("expert", None),
    )
    return jax.shard_map(
        shards, mesh=mesh, in_specs=placed, out_specs=P(("dp", "expert"), None), check_vma=False
    )
```

```python
import functools

import jax
import jax.numpy as jnp
from jax import lax
from jax.experimental import pallas as pl
from jax.experimental.pallas import tpu as pltpu
from jax.sharding import PartitionSpec as P

MESH = pl.DeviceIdType.MESH
epsilon = 1e-05
SIDE = 4
BLOCKS = 16
PACK = 4
RING = 8
OFFSETS = (
    (0, 0), (1, 1), (3, 3), (1, 3),
    (3, 1), (2, 0), (0, 2), (1, 0),
    (3, 0), (0, 1), (0, 3), (2, 1),
    (2, 3), (1, 2), (3, 2), (2, 2),
)
OWN = 11
HOSTS = OFFSETS[:OWN] + tuple(((dx + 2) % SIDE, (dy + 2) % SIDE) for dx, dy in OFFSETS[OWN:])
REMOTE = range(1, BLOCKS - 1)
FFN_GROUPS = ((0, 4), (4, 8), (8, 11), (11, 16))
UPWARD = (4, 3, 4)


def kernel(
    cap, ids_ref, weights_ref, modality_ref, gain_ref, tokens_hbm, gate_hbm, up_hbm, down_hbm, out_hbm,
    tokens, normed, cols, slots, send, recv, res, ret, own_gate, own_up, own_down,
    far_gate, far_up, far_down, act, acc, picks, own_mix, far_mix,
    mixed, load_sem, out_sem, send_sem, recv_sem, back_sem, ret_sem,
    pair_send, pair_recv, ring_send, ring_recv, core_send, core_recv, chain,
):
    rows, width = tokens.shape
    hidden = own_down.shape[0]
    tiles = hidden // 128
    me = lax.axis_index("expert")
    ex, ey = me % SIDE, me // SIDE
    dp = lax.axis_index("dp")
    z, core = dp // 2, dp % 2

    def at_offset(offset, sign):
        dx, dy = offset
        return ((ey + sign * dy + SIDE) % SIDE) * SIDE + (ex + sign * dx + SIDE) % SIDE

    def peer(i, sign):
        return at_offset(HOSTS[i], sign)

    pair = at_offset((2, 2), 1)
    other = z * 2 + 1 - core

    def level(s):
        return (z + s + RING) % RING

    barrier = pltpu.get_barrier_semaphore()
    for i in range(1, OWN):
        pl.semaphore_signal(barrier, inc=1, device_id={"expert": peer(i, 1)}, device_id_type=MESH)
    pl.semaphore_signal(barrier, inc=1, device_id={"expert": pair}, device_id_type=MESH)
    pl.semaphore_signal(barrier, inc=1, device_id={"dp": other}, device_id_type=MESH)

    @pl.when(z < RING - 1)
    def _():
        pl.semaphore_signal(barrier, inc=1, device_id={"dp": level(1) * 2 + core}, device_id_type=MESH)

    @pl.when(z > 0)
    def _():
        pl.semaphore_signal(barrier, inc=1, device_id={"dp": level(-1) * 2 + core}, device_id_type=MESH)

    neighbours = (z + RING - 1) // RING + (2 * (RING - 1) - z) // RING

    load = pltpu.make_async_copy(tokens_hbm, tokens, load_sem.at[0])
    load.start()
    loads = [
        pltpu.make_async_copy(gate_hbm, own_gate, load_sem.at[1]),
        pltpu.make_async_copy(up_hbm, own_up, load_sem.at[2]),
        pltpu.make_async_copy(down_hbm, own_down, load_sem.at[3]),
    ]

    def piece(j, k):
        if j == 2:
            return far_down.at[k]
        return (far_gate, far_up)[j].at[pl.ds(pl.multiple_of(k * 128, 128), 128), :]

    def source_piece(j):
        at = pl.ds(pl.multiple_of(dp * 128, 128), 128)
        return (gate_hbm.at[at, :], up_hbm.at[at, :], down_hbm.at[:, at])[j]

    def pair_copy(j):
        return pltpu.make_async_remote_copy(
            src_ref=source_piece(j), dst_ref=piece(j, dp), send_sem=pair_send.at[j], recv_sem=pair_recv.at[j],
            device_id={"expert": pair}, device_id_type=MESH,
        )

    def ring_copy(j, up, s, origin):
        n = (j * 2 + (0 if up else 1)) * 4 + s - 1
        k = origin * 2 + core
        return pltpu.make_async_remote_copy(
            src_ref=piece(j, k), dst_ref=piece(j, k), send_sem=ring_send.at[n], recv_sem=ring_recv.at[n],
            device_id={"dp": level(1 if up else -1) * 2 + core}, device_id_type=MESH,
        )

    def core_copy(j, n, k):
        return pltpu.make_async_remote_copy(
            src_ref=piece(j, k), dst_ref=piece(j, k), send_sem=core_send.at[j * RING + n],
            recv_sem=core_recv.at[j * RING + n], device_id={"dp": other}, device_id_type=MESH,
        )

    def limit(j, up):
        return UPWARD[j] if up else RING - 1 - UPWARD[j]

    def place(up, s):
        return 0 if s == 0 else (s if up else 4 + s)

    core_slots = {}
    for j in range(3):
        found = [(0, 0)] + [(s, -s) for s in range(1, limit(j, True) + 1)]
        found += [(limit(j, True) + s, s) for s in range(1, limit(j, False) + 1)]
        core_slots[j] = found
    sent = []

    def forward(j, up, s):
        if s == 0:
            pair_copy(j).wait_recv()
            n, origin = 0, level(0)
            copy = ring_copy(j, True, 1, origin)
            copy.start()
            sent.append(copy)
            down = ring_copy(j, False, 1, origin)
            sent.append(down)

            @pl.when(z > 0)
            def _():
                down.start()

        else:
            origin = level(-s if up else s)
            ring_copy(j, up, s, origin).wait_recv()
            n = s if up else limit(j, True) + s
            if s < limit(j, up):
                copy = ring_copy(j, up, s + 1, origin)
                copy.start()
                sent.append(copy)
        copy = core_copy(j, n, origin * 2 + core)
        copy.start()
        sent.append(copy)

    events = [(j, True, 0) for j in range(3)]
    for s in range(1, 5):
        for j in range(3):
            events += [(j, up, s) for up in (True, False) if s <= limit(j, up)]
    pending = iter(events)

    def advance(count):
        for _ in range(count):
            event = next(pending, None)
            if event is not None:
                forward(*event)
            if event == (0, True, 1):

                @pl.when(z == 0)
                def _():
                    for j in range(3):
                        ring_copy(j, False, 1, level(0)).start()

    pl.semaphore_wait(barrier, OWN + 1 + neighbours)
    for j in range(3):
        pair_copy(j).start()
    for copy in loads:
        copy.start()

    @pl.when(z > 0)
    def _():
        pl.semaphore_wait(chain, 1)

    @pl.when(z < RING - 1)
    def _():
        pl.semaphore_signal(chain, inc=1, device_id={"dp": level(1) * 2 + core}, device_id_type=MESH)

    id0, id1 = ids_ref[0:1, :], ids_ref[1:2, :]
    w0, w1 = weights_ref[0:1, :], weights_ref[1:2, :]
    experts = lax.broadcasted_iota(jnp.int32, (BLOCKS, rows), 0)
    is0, is1 = experts == id0, experts == id1
    names = jnp.where(is0 | is1, 1.0, 0.0).astype(jnp.bfloat16)
    before = lax.broadcasted_iota(jnp.int32, (rows, rows), 0) < lax.broadcasted_iota(jnp.int32, (rows, rows), 1)
    earlier = jnp.dot(names, jnp.where(before, 1.0, 0.0).astype(jnp.bfloat16), preferred_element_type=jnp.float32)
    pos0 = jnp.sum(jnp.where(is0, earlier, 0.0), axis=0, keepdims=True)
    pos1 = jnp.sum(jnp.where(is1, earlier, 0.0), axis=0, keepdims=True)
    base0, base1 = jnp.zeros_like(pos0), jnp.zeros_like(pos1)
    for i in range(1, BLOCKS):
        name = at_offset(OFFSETS[i], 1)
        base0 = jnp.where(id0 == name, float(i * cap), base0)
        base1 = jnp.where(id1 == name, float(i * cap), base1)
    slot0, slot1 = base0 + pos0, base1 + pos1
    slots[0:1, :] = slot0.astype(jnp.int32)
    slots[1:2, :] = slot1.astype(jnp.int32)
    kind = modality_ref[...].astype(jnp.float32)
    table = jnp.concatenate([slot0, slot1, w0, w1, kind, kind, kind, kind], axis=0)
    cols[...] = jnp.concatenate([table, jnp.zeros((120, rows), jnp.float32)], axis=0).T

    load.wait()
    step = 64

    def norm_step(r, carry):
        at = pl.ds(pl.multiple_of(r * step, step), step)
        values = tokens[at, :].astype(jnp.float32)
        square = jnp.mean(values * values, axis=1, keepdims=True)
        gains = jnp.where(cols[at, 4:5] == 1.0, gain_ref[1:2, :], gain_ref[0:1, :])
        normed[at, :] = (values * lax.rsqrt(square + epsilon) * gains).astype(jnp.bfloat16)
        return carry

    lax.fori_loop(0, rows // step, norm_step, 0)

    def whole(source, target, sems, rsems, i, device):
        return pltpu.make_async_remote_copy(
            src_ref=source.at[i],
            dst_ref=target.at[i],
            send_sem=sems.at[i],
            recv_sem=rsems.at[i],
            device_id={"expert": device},
            device_id_type=MESH,
        )

    def start_all(source, target, sems, rsems, blocks, sign):
        for i in blocks:
            whole(source, target, sems, rsems, i, peer(i, sign)).start()

    def store(first, last, values, at, remote, local):
        values = values.reshape(last - first, cap, values.shape[-1])
        low, high = max(first, 1), min(last, BLOCKS - 1)
        if first < low:
            local[0:1, :, at] = values[0:1]
        if last > high:
            local[high:last, :, at] = values[high - first :]
        remote[low:high, :, at] = values[low - first : high - first]

    def pack(first, last):
        span = (last - first) * cap
        part = width // 4

        def pick_step(n, carry):
            places = lax.broadcasted_iota(jnp.int32, (cap, rows), 0) + (first + n) * cap
            found = (places == slots[0:1, :]) | (places == slots[1:2, :])
            picks[pl.ds(pl.multiple_of(n * cap, cap), cap), :] = jnp.where(found, 1.0, 0.0).astype(jnp.bfloat16)
            return carry

        lax.fori_loop(0, last - first, pick_step, 0)

        def pack_step(n, carry):
            at = pl.ds(pl.multiple_of(n * part, part), part)
            packed = jnp.dot(picks[0:span, :], normed[:, at], preferred_element_type=jnp.float32).astype(jnp.bfloat16)
            store(first, last, packed, at, send, recv)
            return carry

        lax.fori_loop(0, 4, pack_step, 0)
        start_all(send, recv, send_sem, recv_sem, [i for i in range(first, last) if i in REMOTE], 1)

    def wait_blocks(first, last, returning):
        for i in range(first, last):
            if i in REMOTE:
                if returning:
                    whole(res, ret, back_sem, ret_sem, i, peer(i, -1)).wait_recv()
                else:
                    whole(send, recv, send_sem, recv_sem, i, peer(i, 1)).wait_recv()

    def ffn_hidden(first, last, gate_w, up_w):
        span = (last - first) * cap

        def hidden_step(t, carry):
            at = pl.ds(pl.multiple_of(t * 128, 128), 128)
            flat = recv[first:last].reshape(span, width)
            weights = jnp.concatenate([gate_w[:, at], up_w[:, at]], axis=1)
            both = jnp.dot(flat, weights, preferred_element_type=jnp.float32)
            gate, upper = both[:, :128], both[:, 128:]
            act[0:span, at] = (jax.nn.silu(gate) * upper).astype(jnp.bfloat16)
            return carry

        lax.fori_loop(0, tiles, hidden_step, 0)

    def ffn_down(first, last, down_w):
        span = (last - first) * cap

        def down_step(n, carry):
            at = pl.ds(pl.multiple_of(n * 256, 256), 256)
            done = jnp.dot(act[0:span, :], down_w(n, at), preferred_element_type=jnp.float32)
            store(first, last, done.astype(jnp.bfloat16), at, res, ret)
            return carry

        lax.fori_loop(0, width // 256, down_step, 0)
        start_all(res, ret, back_sem, ret_sem, [i for i in range(first, last) if i in REMOTE], -1)

    def mix_table(first, last, table):
        span = (last - first) * cap

        def table_step(r, carry):
            at = pl.ds(pl.multiple_of(r * step, step), step)
            places = (lax.broadcasted_iota(jnp.int32, (step, span), 1) + first * cap).astype(jnp.float32)
            first_choice = jnp.where(places == cols[at, 0:1], cols[at, 2:3], 0.0)
            second_choice = jnp.where(places == cols[at, 1:2], cols[at, 3:4], 0.0)
            table[at, :] = (first_choice + second_choice).astype(jnp.bfloat16)
            return carry

        lax.fori_loop(0, rows // step, table_step, 0)

    def mix(first, last, table, end):
        span = (last - first) * cap

        def mix_step(n, carry):
            at = pl.ds(pl.multiple_of(n * 256, 256), 256)
            block = ret[first:last, :, at].reshape(span, 256)
            total = jnp.dot(table[...], block, preferred_element_type=jnp.float32)
            if end:
                mixed[:, at] = (acc[:, at] + total).astype(jnp.bfloat16)
                pltpu.make_async_copy(mixed.at[:, at], out_hbm.at[:, at], out_sem.at[n]).start()
            else:
                acc[:, at] = tokens[:, at].astype(jnp.float32) + total
            return carry

        lax.fori_loop(0, width // 256, mix_step, 0)

    def core_wait(j):
        for n, origin in core_slots[j]:
            core_copy(j, n, level(origin) * 2 + 1 - core).wait_recv()

    own_columns = lambda n, at: own_down[:, at]
    far_columns = lambda n, at: jnp.concatenate([far_down[2 * n], far_down[2 * n + 1]], axis=1)

    pack(0, 4)
    advance(1)
    pack(4, 8)
    advance(1)
    pack(8, 12)
    advance(1)
    pack(12, 16)
    advance(2)
    mix_table(0, OWN, own_mix)
    mix_table(OWN, BLOCKS, far_mix)
    for copy in loads:
        copy.wait()
    advance(2)
    wait_blocks(0, 4, False)
    ffn_hidden(0, 4, own_gate, own_up)
    advance(2)
    ffn_down(0, 4, own_columns)
    advance(4)
    wait_blocks(4, 8, False)
    ffn_hidden(4, 8, own_gate, own_up)
    advance(2)
    ffn_down(4, 8, own_columns)
    advance(4)
    wait_blocks(8, OWN, False)
    ffn_hidden(8, OWN, own_gate, own_up)
    advance(2)
    ffn_down(8, OWN, own_columns)
    advance(2)
    core_wait(0)
    core_wait(1)
    wait_blocks(OWN, BLOCKS, False)
    ffn_hidden(OWN, BLOCKS, far_gate, far_up)
    advance(1)
    core_wait(2)
    ffn_down(OWN, BLOCKS, far_columns)
    wait_blocks(0, OWN, True)
    mix(0, OWN, own_mix, False)
    wait_blocks(OWN, BLOCKS, True)
    mix(OWN, BLOCKS, far_mix, True)

    for i in REMOTE:
        whole(send, recv, send_sem, recv_sem, i, peer(i, 1)).wait_send()
        whole(res, ret, back_sem, ret_sem, i, peer(i, -1)).wait_send()
    for j in range(3):
        pair_copy(j).wait_send()
    for copy in sent:
        copy.wait_send()
    for n in range(width // 256):
        at = pl.ds(n * 256, 256)
        pltpu.make_async_copy(mixed.at[:, at], out_hbm.at[:, at], out_sem.at[n]).wait()


def hand_over(source, target, held, in_sem, out_sem):
    count = held.shape[0]
    reads = [pltpu.make_async_copy(source.at[n], held.at[n], in_sem.at[n]) for n in range(count)]
    writes = [pltpu.make_async_copy(held.at[n], target.at[n], out_sem.at[n]) for n in range(count)]
    for read in reads:
        read.start()
    for read, write in zip(reads, writes):
        read.wait()
        write.start()
    for write in writes:
        write.wait()


def shards(tokens, modality, expert_ids, route_weights, norm_gain, gate_weight, up_weight, down_weight):
    rows, width = tokens.shape
    fanout = expert_ids.shape[1]
    hidden = down_weight.shape[0]
    cap = min(rows, rows * fanout * 5 // (4 * BLOCKS))
    anywhere = pl.BlockSpec(memory_space=pl.ANY)
    vmem = pl.BlockSpec(memory_space=pltpu.VMEM)
    block = pltpu.VMEM((BLOCKS, cap, width), jnp.bfloat16)
    sems = pltpu.SemaphoreType.DMA((BLOCKS,))
    dma = pltpu.SemaphoreType.DMA
    longest = max(last - first for first, last in FFN_GROUPS)
    result = pl.pallas_call(
        functools.partial(kernel, cap),
        out_shape=jax.ShapeDtypeStruct((rows, width), jnp.bfloat16),
        in_specs=[vmem, vmem, vmem, vmem, anywhere, anywhere, anywhere, anywhere],
        out_specs=anywhere,
        scratch_shapes=[
            pltpu.VMEM((rows, width), jnp.bfloat16),
            pltpu.VMEM((rows, width), jnp.bfloat16),
            pltpu.VMEM((rows, 128), jnp.float32),
            pltpu.VMEM((8, rows), jnp.int32),
            block, block, block, block,
            pltpu.VMEM((width, hidden), jnp.bfloat16),
            pltpu.VMEM((width, hidden), jnp.bfloat16),
            pltpu.VMEM((hidden, width), jnp.bfloat16),
            pltpu.VMEM((width, hidden), jnp.bfloat16),
            pltpu.VMEM((width, hidden), jnp.bfloat16),
            pltpu.VMEM((width // 128, hidden, 128), jnp.bfloat16),
            pltpu.VMEM((longest * cap, hidden), jnp.bfloat16),
            pltpu.VMEM((rows, width), jnp.float32),
            pltpu.VMEM((PACK * cap, rows), jnp.bfloat16),
            pltpu.VMEM((rows, OWN * cap), jnp.bfloat16),
            pltpu.VMEM((rows, (BLOCKS - OWN) * cap), jnp.bfloat16),
            pltpu.VMEM((rows, width), jnp.bfloat16),
            dma((4,)),
            dma((width // 256,)),
            sems, sems, sems, sems,
            dma((3,)), dma((3,)), dma((24,)), dma((24,)), dma((24,)), dma((24,)),
            pltpu.SemaphoreType.REGULAR,
        ],
        compiler_params=pltpu.CompilerParams(
            collective_id=0, has_side_effects=True, vmem_limit_bytes=63 * 1024 * 1024
        ),
    )(expert_ids.T, route_weights.T, modality[None, :], norm_gain, tokens, gate_weight, up_weight, down_weight)
    pieces = 8
    shape = (pieces, rows // pieces, width)
    return pl.pallas_call(
        hand_over,
        out_shape=jax.ShapeDtypeStruct(shape, jnp.bfloat16),
        in_specs=[anywhere],
        out_specs=anywhere,
        scratch_shapes=[pltpu.VMEM(shape, jnp.bfloat16), dma((pieces,)), dma((pieces,))],
    )(result.reshape(shape)).reshape(rows, width)


def solution(mesh):
    placed = (
        P(("dp", "expert"), None),
        P(("dp", "expert")),
        P(("dp", "expert"), None),
        P(("dp", "expert"), None),
        P(),
        P(None, "expert"),
        P(None, "expert"),
        P("expert", None),
    )
    return jax.shard_map(
        shards, mesh=mesh, in_specs=placed, out_specs=P(("dp", "expert"), None), check_vma=False
    )
```

```python
import functools

import jax
import jax.numpy as jnp
from jax import lax
from jax.experimental import pallas as pl
from jax.experimental.pallas import tpu as pltpu
from jax.sharding import PartitionSpec as P

MESH = pl.DeviceIdType.MESH
epsilon = 1e-05
SIDE = 4
BLOCKS = 16
PACK = 4
RING = 8
OFFSETS = (
    (0, 0), (1, 1), (3, 3), (1, 3),
    (3, 1), (2, 0), (0, 2), (1, 0),
    (3, 0), (0, 1), (0, 3), (2, 1),
    (2, 3), (1, 2), (3, 2), (2, 2),
)
OWN = 11
HOSTS = OFFSETS[:OWN] + tuple(((dx + 2) % SIDE, (dy + 2) % SIDE) for dx, dy in OFFSETS[OWN:])
REMOTE = range(1, BLOCKS - 1)
FFN_GROUPS = ((0, 4), (4, 8), (8, 11), (11, 16))
UPWARD = (4, 3, 4)


def kernel(
    cap, ids_ref, weights_ref, modality_ref, gain_ref, tokens_hbm, gate_hbm, up_hbm, down_hbm, out_hbm,
    tokens, normed, cols, slots, send, recv, res, ret, own_gate, own_up, own_down,
    far_gate, far_up, far_down, act, acc, picks, own_mix, far_mix,
    mixed, load_sem, out_sem, send_sem, recv_sem, back_sem, ret_sem,
    pair_send, pair_recv, ring_send, ring_recv, core_send, core_recv,
):
    rows, width = tokens.shape
    hidden = own_down.shape[0]
    tiles = hidden // 128
    me = lax.axis_index("expert")
    ex, ey = me % SIDE, me // SIDE
    dp = lax.axis_index("dp")
    z, core = dp // 2, dp % 2

    def at_offset(offset, sign):
        dx, dy = offset
        return ((ey + sign * dy + SIDE) % SIDE) * SIDE + (ex + sign * dx + SIDE) % SIDE

    def peer(i, sign):
        return at_offset(HOSTS[i], sign)

    pair = at_offset((2, 2), 1)
    other = z * 2 + 1 - core

    def level(s):
        return (z + s + RING) % RING

    barrier = pltpu.get_barrier_semaphore()
    for i in range(1, OWN):
        pl.semaphore_signal(barrier, inc=1, device_id={"expert": peer(i, 1)}, device_id_type=MESH)
    pl.semaphore_signal(barrier, inc=1, device_id={"expert": pair}, device_id_type=MESH)
    for s in (1, -1):
        pl.semaphore_signal(barrier, inc=1, device_id={"dp": level(s) * 2 + core}, device_id_type=MESH)
    pl.semaphore_signal(barrier, inc=1, device_id={"dp": other}, device_id_type=MESH)

    load = pltpu.make_async_copy(tokens_hbm, tokens, load_sem.at[0])
    load.start()
    loads = [
        pltpu.make_async_copy(gate_hbm, own_gate, load_sem.at[1]),
        pltpu.make_async_copy(up_hbm, own_up, load_sem.at[2]),
        pltpu.make_async_copy(down_hbm, own_down, load_sem.at[3]),
    ]

    def piece(j, k):
        if j == 2:
            return far_down.at[k]
        return (far_gate, far_up)[j].at[pl.ds(pl.multiple_of(k * 128, 128), 128), :]

    def source_piece(j):
        at = pl.ds(pl.multiple_of(dp * 128, 128), 128)
        return (gate_hbm.at[at, :], up_hbm.at[at, :], down_hbm.at[:, at])[j]

    def pair_copy(j):
        return pltpu.make_async_remote_copy(
            src_ref=source_piece(j), dst_ref=piece(j, dp), send_sem=pair_send.at[j], recv_sem=pair_recv.at[j],
            device_id={"expert": pair}, device_id_type=MESH,
        )

    def ring_copy(j, up, s, origin):
        n = (j * 2 + (0 if up else 1)) * 4 + s - 1
        k = origin * 2 + core
        return pltpu.make_async_remote_copy(
            src_ref=piece(j, k), dst_ref=piece(j, k), send_sem=ring_send.at[n], recv_sem=ring_recv.at[n],
            device_id={"dp": level(1 if up else -1) * 2 + core}, device_id_type=MESH,
        )

    def core_copy(j, n, k):
        return pltpu.make_async_remote_copy(
            src_ref=piece(j, k), dst_ref=piece(j, k), send_sem=core_send.at[j * RING + n],
            recv_sem=core_recv.at[j * RING + n], device_id={"dp": other}, device_id_type=MESH,
        )

    def limit(j, up):
        return UPWARD[j] if up else RING - 1 - UPWARD[j]

    def place(up, s):
        return 0 if s == 0 else (s if up else 4 + s)

    core_slots = {}
    for j in range(3):
        found = [(0, 0)] + [(s, -s) for s in range(1, limit(j, True) + 1)]
        found += [(limit(j, True) + s, s) for s in range(1, limit(j, False) + 1)]
        core_slots[j] = found
    sent = []

    def forward(j, up, s):
        if s == 0:
            pair_copy(j).wait_recv()
            n, origin = 0, level(0)
            for way in (True, False):
                copy = ring_copy(j, way, 1, origin)
                copy.start()
                sent.append(copy)
        else:
            origin = level(-s if up else s)
            ring_copy(j, up, s, origin).wait_recv()
            n = s if up else limit(j, True) + s
            if s < limit(j, up):
                copy = ring_copy(j, up, s + 1, origin)
                copy.start()
                sent.append(copy)
        copy = core_copy(j, n, origin * 2 + core)
        copy.start()
        sent.append(copy)

    events = [(j, True, 0) for j in range(3)]
    for s in range(1, 5):
        for j in range(3):
            events += [(j, up, s) for up in (True, False) if s <= limit(j, up)]
    pending = iter(events)

    def advance(count):
        for _ in range(count):
            event = next(pending, None)
            if event is not None:
                forward(*event)

    pl.semaphore_wait(barrier, OWN + 3)
    for j in range(3):
        pair_copy(j).start()
    for copy in loads:
        copy.start()

    id0, id1 = ids_ref[0:1, :], ids_ref[1:2, :]
    w0, w1 = weights_ref[0:1, :], weights_ref[1:2, :]
    experts = lax.broadcasted_iota(jnp.int32, (BLOCKS, rows), 0)
    is0, is1 = experts == id0, experts == id1
    names = jnp.where(is0 | is1, 1.0, 0.0).astype(jnp.bfloat16)
    before = lax.broadcasted_iota(jnp.int32, (rows, rows), 0) < lax.broadcasted_iota(jnp.int32, (rows, rows), 1)
    earlier = jnp.dot(names, jnp.where(before, 1.0, 0.0).astype(jnp.bfloat16), preferred_element_type=jnp.float32)
    pos0 = jnp.sum(jnp.where(is0, earlier, 0.0), axis=0, keepdims=True)
    pos1 = jnp.sum(jnp.where(is1, earlier, 0.0), axis=0, keepdims=True)
    base0, base1 = jnp.zeros_like(pos0), jnp.zeros_like(pos1)
    for i in range(1, BLOCKS):
        name = at_offset(OFFSETS[i], 1)
        base0 = jnp.where(id0 == name, float(i * cap), base0)
        base1 = jnp.where(id1 == name, float(i * cap), base1)
    slot0, slot1 = base0 + pos0, base1 + pos1
    slots[0:1, :] = slot0.astype(jnp.int32)
    slots[1:2, :] = slot1.astype(jnp.int32)
    kind = modality_ref[...].astype(jnp.float32)
    table = jnp.concatenate([slot0, slot1, w0, w1, kind, kind, kind, kind], axis=0)
    cols[...] = jnp.concatenate([table, jnp.zeros((120, rows), jnp.float32)], axis=0).T

    load.wait()
    step = 64

    def norm_step(r, carry):
        at = pl.ds(pl.multiple_of(r * step, step), step)
        values = tokens[at, :].astype(jnp.float32)
        square = jnp.mean(values * values, axis=1, keepdims=True)
        gains = jnp.where(cols[at, 4:5] == 1.0, gain_ref[1:2, :], gain_ref[0:1, :])
        normed[at, :] = (values * lax.rsqrt(square + epsilon) * gains).astype(jnp.bfloat16)
        return carry

    lax.fori_loop(0, rows // step, norm_step, 0)

    def whole(source, target, sems, rsems, i, device):
        return pltpu.make_async_remote_copy(
            src_ref=source.at[i],
            dst_ref=target.at[i],
            send_sem=sems.at[i],
            recv_sem=rsems.at[i],
            device_id={"expert": device},
            device_id_type=MESH,
        )

    def start_all(source, target, sems, rsems, blocks, sign):
        for i in blocks:
            whole(source, target, sems, rsems, i, peer(i, sign)).start()

    def store(first, last, values, at, remote, local):
        values = values.reshape(last - first, cap, values.shape[-1])
        low, high = max(first, 1), min(last, BLOCKS - 1)
        if first < low:
            local[0:1, :, at] = values[0:1]
        if last > high:
            local[high:last, :, at] = values[high - first :]
        remote[low:high, :, at] = values[low - first : high - first]

    def pack(first, last):
        span = (last - first) * cap
        part = width // 4

        def pick_step(n, carry):
            places = lax.broadcasted_iota(jnp.int32, (cap, rows), 0) + (first + n) * cap
            found = (places == slots[0:1, :]) | (places == slots[1:2, :])
            picks[pl.ds(pl.multiple_of(n * cap, cap), cap), :] = jnp.where(found, 1.0, 0.0).astype(jnp.bfloat16)
            return carry

        lax.fori_loop(0, last - first, pick_step, 0)

        def pack_step(n, carry):
            at = pl.ds(pl.multiple_of(n * part, part), part)
            packed = jnp.dot(picks[0:span, :], normed[:, at], preferred_element_type=jnp.float32).astype(jnp.bfloat16)
            store(first, last, packed, at, send, recv)
            return carry

        lax.fori_loop(0, 4, pack_step, 0)
        start_all(send, recv, send_sem, recv_sem, [i for i in range(first, last) if i in REMOTE], 1)

    def wait_blocks(first, last, returning):
        for i in range(first, last):
            if i in REMOTE:
                if returning:
                    whole(res, ret, back_sem, ret_sem, i, peer(i, -1)).wait_recv()
                else:
                    whole(send, recv, send_sem, recv_sem, i, peer(i, 1)).wait_recv()

    def ffn_hidden(first, last, gate_w, up_w):
        span = (last - first) * cap

        def hidden_step(t, carry):
            at = pl.ds(pl.multiple_of(t * 128, 128), 128)
            flat = recv[first:last].reshape(span, width)
            weights = jnp.concatenate([gate_w[:, at], up_w[:, at]], axis=1)
            both = jnp.dot(flat, weights, preferred_element_type=jnp.float32)
            gate, upper = both[:, :128], both[:, 128:]
            act[0:span, at] = (jax.nn.silu(gate) * upper).astype(jnp.bfloat16)
            return carry

        lax.fori_loop(0, tiles, hidden_step, 0)

    def ffn_down(first, last, down_w):
        span = (last - first) * cap

        def down_step(n, carry):
            at = pl.ds(pl.multiple_of(n * 256, 256), 256)
            done = jnp.dot(act[0:span, :], down_w(n, at), preferred_element_type=jnp.float32)
            store(first, last, done.astype(jnp.bfloat16), at, res, ret)
            return carry

        lax.fori_loop(0, width // 256, down_step, 0)
        start_all(res, ret, back_sem, ret_sem, [i for i in range(first, last) if i in REMOTE], -1)

    def mix_table(first, last, table):
        span = (last - first) * cap

        def table_step(r, carry):
            at = pl.ds(pl.multiple_of(r * step, step), step)
            places = (lax.broadcasted_iota(jnp.int32, (step, span), 1) + first * cap).astype(jnp.float32)
            first_choice = jnp.where(places == cols[at, 0:1], cols[at, 2:3], 0.0)
            second_choice = jnp.where(places == cols[at, 1:2], cols[at, 3:4], 0.0)
            table[at, :] = (first_choice + second_choice).astype(jnp.bfloat16)
            return carry

        lax.fori_loop(0, rows // step, table_step, 0)

    def mix(first, last, table, end):
        span = (last - first) * cap

        def mix_step(n, carry):
            at = pl.ds(pl.multiple_of(n * 256, 256), 256)
            block = ret[first:last, :, at].reshape(span, 256)
            total = jnp.dot(table[...], block, preferred_element_type=jnp.float32)
            if end:
                mixed[:, at] = (acc[:, at] + total).astype(jnp.bfloat16)
                pltpu.make_async_copy(mixed.at[:, at], out_hbm.at[:, at], out_sem.at[n]).start()
            else:
                acc[:, at] = tokens[:, at].astype(jnp.float32) + total
            return carry

        lax.fori_loop(0, width // 256, mix_step, 0)

    def core_wait(j):
        for n, origin in core_slots[j]:
            core_copy(j, n, level(origin) * 2 + 1 - core).wait_recv()

    own_columns = lambda n, at: own_down[:, at]
    far_columns = lambda n, at: jnp.concatenate([far_down[2 * n], far_down[2 * n + 1]], axis=1)

    pack(0, 4)
    advance(1)
    pack(4, 8)
    advance(1)
    pack(8, 12)
    advance(1)
    pack(12, 16)
    advance(2)
    mix_table(0, OWN, own_mix)
    mix_table(OWN, BLOCKS, far_mix)
    for copy in loads:
        copy.wait()
    advance(2)
    wait_blocks(0, 4, False)
    advance(1)
    ffn_hidden(0, 4, own_gate, own_up)
    advance(2)
    ffn_down(0, 4, own_columns)
    advance(4)
    wait_blocks(4, 8, False)
    advance(1)
    ffn_hidden(4, 8, own_gate, own_up)
    advance(2)
    ffn_down(4, 8, own_columns)
    advance(3)
    wait_blocks(8, OWN, False)
    ffn_hidden(8, OWN, own_gate, own_up)
    advance(2)
    ffn_down(8, OWN, own_columns)
    advance(2)
    core_wait(0)
    core_wait(1)
    wait_blocks(OWN, BLOCKS, False)
    ffn_hidden(OWN, BLOCKS, far_gate, far_up)
    advance(1)
    core_wait(2)
    ffn_down(OWN, BLOCKS, far_columns)
    wait_blocks(0, OWN, True)
    mix(0, OWN, own_mix, False)
    wait_blocks(OWN, BLOCKS, True)
    mix(OWN, BLOCKS, far_mix, True)

    for i in REMOTE:
        whole(send, recv, send_sem, recv_sem, i, peer(i, 1)).wait_send()
        whole(res, ret, back_sem, ret_sem, i, peer(i, -1)).wait_send()
    for j in range(3):
        pair_copy(j).wait_send()
    for copy in sent:
        copy.wait_send()
    for n in range(width // 256):
        at = pl.ds(n * 256, 256)
        pltpu.make_async_copy(mixed.at[:, at], out_hbm.at[:, at], out_sem.at[n]).wait()


def hand_over(source, target, held, in_sem, out_sem):
    count = held.shape[0]
    reads = [pltpu.make_async_copy(source.at[n], held.at[n], in_sem.at[n]) for n in range(count)]
    writes = [pltpu.make_async_copy(held.at[n], target.at[n], out_sem.at[n]) for n in range(count)]
    for read in reads:
        read.start()
    for read, write in zip(reads, writes):
        read.wait()
        write.start()
    for write in writes:
        write.wait()


def shards(tokens, modality, expert_ids, route_weights, norm_gain, gate_weight, up_weight, down_weight):
    rows, width = tokens.shape
    fanout = expert_ids.shape[1]
    hidden = down_weight.shape[0]
    cap = min(rows, rows * fanout * 5 // (4 * BLOCKS))
    anywhere = pl.BlockSpec(memory_space=pl.ANY)
    vmem = pl.BlockSpec(memory_space=pltpu.VMEM)
    block = pltpu.VMEM((BLOCKS, cap, width), jnp.bfloat16)
    sems = pltpu.SemaphoreType.DMA((BLOCKS,))
    dma = pltpu.SemaphoreType.DMA
    longest = max(last - first for first, last in FFN_GROUPS)
    result = pl.pallas_call(
        functools.partial(kernel, cap),
        out_shape=jax.ShapeDtypeStruct((rows, width), jnp.bfloat16),
        in_specs=[vmem, vmem, vmem, vmem, anywhere, anywhere, anywhere, anywhere],
        out_specs=anywhere,
        scratch_shapes=[
            pltpu.VMEM((rows, width), jnp.bfloat16),
            pltpu.VMEM((rows, width), jnp.bfloat16),
            pltpu.VMEM((rows, 128), jnp.float32),
            pltpu.VMEM((8, rows), jnp.int32),
            block, block, block, block,
            pltpu.VMEM((width, hidden), jnp.bfloat16),
            pltpu.VMEM((width, hidden), jnp.bfloat16),
            pltpu.VMEM((hidden, width), jnp.bfloat16),
            pltpu.VMEM((width, hidden), jnp.bfloat16),
            pltpu.VMEM((width, hidden), jnp.bfloat16),
            pltpu.VMEM((width // 128, hidden, 128), jnp.bfloat16),
            pltpu.VMEM((longest * cap, hidden), jnp.bfloat16),
            pltpu.VMEM((rows, width), jnp.float32),
            pltpu.VMEM((PACK * cap, rows), jnp.bfloat16),
            pltpu.VMEM((rows, OWN * cap), jnp.bfloat16),
            pltpu.VMEM((rows, (BLOCKS - OWN) * cap), jnp.bfloat16),
            pltpu.VMEM((rows, width), jnp.bfloat16),
            dma((4,)),
            dma((width // 256,)),
            sems, sems, sems, sems,
            dma((3,)), dma((3,)), dma((24,)), dma((24,)), dma((24,)), dma((24,)),
        ],
        compiler_params=pltpu.CompilerParams(
            collective_id=0, has_side_effects=True, vmem_limit_bytes=63 * 1024 * 1024
        ),
    )(expert_ids.T, route_weights.T, modality[None, :], norm_gain, tokens, gate_weight, up_weight, down_weight)
    pieces = 8
    shape = (pieces, rows // pieces, width)
    return pl.pallas_call(
        hand_over,
        out_shape=jax.ShapeDtypeStruct(shape, jnp.bfloat16),
        in_specs=[anywhere],
        out_specs=anywhere,
        scratch_shapes=[pltpu.VMEM(shape, jnp.bfloat16), dma((pieces,)), dma((pieces,))],
    )(result.reshape(shape)).reshape(rows, width)


def solution(mesh):
    placed = (
        P(("dp", "expert"), None),
        P(("dp", "expert")),
        P(("dp", "expert"), None),
        P(("dp", "expert"), None),
        P(),
        P(None, "expert"),
        P(None, "expert"),
        P("expert", None),
    )
    return jax.shard_map(
        shards, mesh=mesh, in_specs=placed, out_specs=P(("dp", "expert"), None), check_vma=False
    )
```
